256 devices in a mesh: seq: 64 (over z, y, core), feat: 4 (over x).
Axes of the slice: x: 4, y: 4, z: 8, core: 2. Of those that a mesh axis runs over, the one named last changes fastest.
Arguments:
- hidden_in: bfloat16 [4, 16384, 2048], P(None, 'seq'), may hold values from -6 to 6
- w_query: bfloat16 [2048, 256], replicated, may hold values from -0.125 to 0.125
- w_key: bfloat16 [2048, 256], replicated, may hold values from -0.125 to 0.125
- w_value: bfloat16 [2048, 2048], P(None, 'feat'), may hold values from -0.125 to 0.125
- lengths: int32 [4], replicated, may hold values from 8192 to 16384, as said below
- owners: int32 [4], replicated, may hold values from 0 to 63
Outputs:
- mixed: bfloat16 [4, 16384, 2048], P(None, 'seq', 'feat')
- state_quad: float32 [64, 4, 16, 256, 128], P('seq', None, None, 'feat')
- state_low: float32 [64, 4, 16, 17, 128], P('seq', None, 'feat')
- norm_quad: float32 [64, 4, 16, 256], P('seq', None, None, 'feat')
- norm_low: float32 [64, 4, 16, 17], P('seq', None, 'feat')
The draws below stay inside these ranges and needn't reach their ends.
Inputs may be any that keep to these rules, and one draw needn't show every extreme that they name: `lengths`: every prompt holds 8192 to 16384 live tokens, and some prompt holds exactly 16384. `owners`: several prompts may share a decoding device.
All inputs are finite; a program needn't handle non-finite values.
Results may differ from the reference program's by a relative error of at most 0.0085.
Values may be sent and summed in bfloat16 or wider, within the bound.
A program may use at most 256 MiB of HBM per device.

```python
import jax
import jax.numpy as jnp
from jax import lax

D = 2048
H = 16
HD = 128
FD = 16
PROMPTS = 4
SPAN = 256
LENGTH = 16384
N_SEQ = 64


def draw_lengths(key, part):
    first_key, second_key = jax.random.split(jax.random.fold_in(key, 11))
    drawn = jax.random.randint(first_key, (PROMPTS,), LENGTH // 2, LENGTH + 1)
    longest = jax.random.randint(second_key, (), 0, PROMPTS)
    return jnp.where(jnp.arange(PROMPTS) == longest, LENGTH, drawn).astype(jnp.int32)


def touch_ends(array, stream_key, least, top_value):
    dims = array.shape
    spot = [jax.random.randint(jax.random.fold_in(stream_key, axis), (), 0, dims[axis]) for axis in range(len(dims))]
    array = array.at[tuple(spot)].set(least)
    longest = dims.index(max(dims))
    spot[longest] = (spot[longest] + 1) % dims[longest]
    return array.at[tuple(spot)].set(top_value)


def levels(stream_key, shape, shards, low, largest):
    def one(axis_at, parts):
        draws = jax.random.uniform(jax.random.fold_in(jax.random.fold_in(stream_key, 6), axis_at), (parts,), jnp.float32, low / len(shards), largest / len(shards))
        return jnp.repeat(jnp.exp(draws), shape[axis_at] // parts).reshape((-1,) + (1,) * (len(shape) - axis_at - 1))

    level = one(*shards[0])
    for cut in shards[1:]:
        level = level * one(*cut)
    return level


def noise(own_key, shape, spread, most, cuts=(), held_as=jnp.bfloat16):
    array = jax.random.normal(own_key, shape, jnp.float32) * spread
    if len(cuts) > 0:
        array = levels(own_key, shape, cuts, -0.22, 0.18) * array
    return jnp.clip(array, min=-most, max=most).astype(held_as)


def setup_inputs(seed: int = 0) -> dict:
    streams_of = jax.random.split(jax.random.key(seed), 7)
    hidden_in = noise(streams_of[0], (PROMPTS, LENGTH, D), 1.0, 6.0, ((1, 64),))
    w_query = noise(streams_of[1], (D, H * FD), D ** -0.5, 0.125)
    w_key = noise(streams_of[2], (D, H * FD), D ** -0.5, 0.125)
    w_value = noise(streams_of[3], (D, D), D ** -0.5, 0.125, ((1, 4),))
    lengths = draw_lengths(jax.random.fold_in(streams_of[6], 71), 0)
    owners = touch_ends(jax.random.randint(streams_of[5], (PROMPTS,), 0, N_SEQ), jax.random.fold_in(streams_of[5], 1), 0, N_SEQ - 1).astype(jnp.int32)
    return dict(hidden_in=hidden_in, w_query=w_query, w_key=w_key, w_value=w_value, lengths=lengths, owners=owners)


NORM_FLOOR = 0.0001

def low_features(inputs):
    constant = jnp.ones(inputs.shape[:-1] + (1,), jnp.float32)
    return jnp.concatenate([constant, inputs * FD ** (-0.25)], axis=-1)

def quad_features(leading, inputs):
    products = leading[..., :, None] * inputs[..., None, :]
    return products.reshape(inputs.shape[:-1] + (leading.shape[-1] * inputs.shape[-1],)) * (2.0 * FD) ** (-0.5)

def reference(hidden_in, w_query, w_key, w_value, lengths, owners):
    highest = lax.Precision.HIGHEST
    n_blocks = LENGTH // SPAN

    def per_prompt(prompt_item):
        tokens, length = prompt_item
        queries = jnp.dot(tokens, w_query, preferred_element_type=jnp.float32).astype(jnp.bfloat16)
        key_rows = jnp.dot(tokens, w_key, preferred_element_type=jnp.float32).astype(jnp.bfloat16)
        values = jnp.dot(tokens, w_value, preferred_element_type=jnp.float32).astype(jnp.bfloat16)
        query_blocks = queries.astype(jnp.float32).reshape(n_blocks, SPAN, H, FD)
        key_blocks = key_rows.astype(jnp.float32).reshape(n_blocks, SPAN, H, FD)
        value_blocks = values.astype(jnp.float32).reshape(n_blocks, SPAN, H, HD)
        starts = jnp.arange(n_blocks, dtype=jnp.int32) * SPAN
        causal = (jnp.arange(SPAN)[:, None] >= jnp.arange(SPAN)[None, :]).astype(jnp.float32)

        def advance(carried, block_data):
            state_lo, state_qu, norm_lo, norm_qu = carried
            query_blk, key_blk, value_blk, start = block_data
            positions = start + jnp.arange(SPAN, dtype=jnp.int32)
            live_mask = (positions < length).astype(jnp.float32)
            query_low = low_features(query_blk)
            query_quad = quad_features(query_blk, query_blk)
            key_low = low_features(key_blk) * live_mask[:, None, None]
            key_quad = quad_features(key_blk, key_blk) * live_mask[:, None, None]
            numerator = jnp.einsum('thf,hfd->thd', query_low, state_lo, precision=highest)
            numerator = numerator + jnp.einsum('thf,hfd->thd', query_quad, state_qu, precision=highest)
            denominator = jnp.einsum('thf,hf->th', query_low, norm_lo, precision=highest)
            denominator = denominator + jnp.einsum('thf,hf->th', query_quad, norm_qu, precision=highest)
            scores = jnp.einsum('thf,uhf->htu', query_blk, key_blk, precision=highest)
            kernel = 1.0 + scores * FD ** (-0.5) + scores * scores * (0.5 / FD)
            weight = kernel * causal[None, :, :] * live_mask[None, None, :]
            numerator = numerator + jnp.einsum('htu,uhd->thd', weight, value_blk, precision=highest)
            denominator = denominator + lax.optimization_barrier(jnp.sum(weight, axis=2)).T
            attended = numerator / denominator[:, :, None] * live_mask[:, None, None]
            new_carried = (state_lo + jnp.einsum('thf,thd->hfd', key_low, value_blk, precision=highest), state_qu + jnp.einsum('thf,thd->hfd', key_quad, value_blk, precision=highest), norm_lo + lax.optimization_barrier(jnp.sum(key_low, axis=0)), norm_qu + lax.optimization_barrier(jnp.sum(key_quad, axis=0)))
            return (new_carried, attended.reshape(SPAN, H * HD))
        initial = (jnp.zeros((H, FD + 1, HD), jnp.float32), jnp.zeros((H, FD * FD, HD), jnp.float32), jnp.zeros((H, FD + 1), jnp.float32), jnp.zeros((H, FD * FD), jnp.float32))
        finals, attended = lax.scan(advance, initial, (query_blocks, key_blocks, value_blocks, starts))
        attended = attended.reshape(LENGTH, H * HD)
        mean_square = lax.optimization_barrier(jnp.mean(attended * attended, axis=-1))
        mixed = (attended * lax.rsqrt(mean_square + NORM_FLOOR)[:, None]).astype(jnp.bfloat16)
        return (mixed, finals)
    mixed, finals = lax.map(per_prompt, (hidden_in, lengths))
    final_low, final_quad, final_lnorm, final_qnorm = finals
    owner_table = (jnp.arange(N_SEQ, dtype=jnp.int32)[:, None] == owners[None, :]).astype(jnp.float32)
    state_quad = owner_table[:, :, None, None, None] * final_quad[None]
    state_low = owner_table[:, :, None, None, None] * final_low[None]
    norm_quad = owner_table[:, :, None, None] * final_qnorm[None]
    norm_low = owner_table[:, :, None, None] * final_lnorm[None]
    return (mixed, state_quad, state_low, norm_quad, norm_low)
```

```python
import functools

import jax
import jax.numpy as jnp
import numpy as np
from jax import lax
from jax.experimental import pallas as pl
from jax.experimental.pallas import tpu as pltpu
from jax.sharding import Mesh
from jax.sharding import PartitionSpec as P

MESH = pl.DeviceIdType.MESH
F32, BF16 = jnp.float32, jnp.bfloat16
FD = 16
ROWS = 160
LIN, ONE, NORM = 136, 152, 153
HD = 128
NORM_FLOOR = 0.0001
HL = 4
SEQ = ("z", "y", "c")


def packed_pairs():
    pairs = [(i, (i + d) % FD, d) for d in range(8) for i in range(FD)]
    return pairs + [(i, i + 8, 8) for i in range(8)]


def row_of(i, j):
    d = (j - i) % FD
    if d < 8:
        return d * FD + i
    if d == 8:
        return 8 * FD + min(i, j)
    return (FD - d) * FD + j


@functools.cache
def tables(nx):
    ek = np.zeros((2, HL, ROWS, 128), np.float32)
    eq = np.zeros((2, HL, 128, ROWS), np.float32)
    for h in range(HL):
        for r, (i, j, d) in enumerate(packed_pairs()):
            ek[0, h, r, h * FD + i] = ek[1, h, r, h * FD + j] = 1.0
            eq[0, h, h * FD + i, r] = 1.0 / 32 if d == 0 else 1.0 / 16
            eq[1, h, h * FD + j, r] = 1.0
        for i in range(FD):
            ek[0, h, LIN + i, h * FD + i] = ek[1, h, LIN + i, 65] = 1.0
            eq[0, h, h * FD + i, LIN + i] = 0.25
            eq[1, h, 65, LIN + i] = 1.0
        ek[0, h, ONE, 64] = ek[1, h, ONE, 64] = 1.0
        eq[0, h, 65, ONE] = eq[1, h, 65, ONE] = 1.0
    own = FD // nx
    sel = np.zeros((nx, own * FD + 16, ROWS), np.float32)
    for x in range(nx):
        for ii in range(own):
            for j in range(FD):
                sel[x, ii * FD + j, row_of(x * own + ii, j)] = 1.0
        sel[x, own * FD, NORM] = sel[x, own * FD + 1, NORM + 1] = 1.0
    return (
        ek.reshape(2 * HL * ROWS, 128).astype(BF16),
        eq.reshape(2 * HL, 128, ROWS).astype(BF16),
        sel.reshape(-1, ROWS).astype(BF16),
    )


def dot(a, b, ca=1, cb=0):
    return lax.dot_general(a, b, (((ca,), (cb,)), ((), ())), preferred_element_type=F32)


def kernel(
    sizes, len_ref, hid_hbm, wv_hbm, wk_hbm, wq_hbm, ek_hbm, eq_hbm, sel_hbm, mixed_hbm, fx_hbm, low_hbm,
    hid, wv, wkq, ek, eq, sel, val, keyt, qry, phi, nself, dself, att, mixed, cm, sq, rsq,
    loc, r0, csum, ry, tz, rz, pz, rpz, tt, rtt, py, rpy, pc, rpc, fxs, fxa, lowa,
    lsem, hsem, s0, v0, sy, vy, sz, vz, sz2, vz2, sz3, vz3, sy2, vy2, s02, v02,
    sx, vx, sy3, vy3, sy4, vy4, s3, v3, sx2, vx2, osem,
):
    nz, ny, nc, nx, span, width = sizes
    zr = 2 * ROWS // nz
    z, y, c, x = (lax.axis_index(a) for a in ("z", "y", "c", "x"))
    other = 1 - c
    pos0 = ((z * ny + y) * nc + c) * span

    col = pl.multiple_of((x * (HL * FD)) // 128 * 128, 128)
    shift = lax.rem(x * (HL * FD), 128)

    def hid_copy(p):
        return pltpu.make_async_copy(hid_hbm.at[p], hid.at[p], hsem.at[p])

    loads = [
        pltpu.make_async_copy(wk_hbm.at[:, pl.ds(col, 128)], wkq.at[:, pl.ds(0, 128)], lsem.at[0]),
        pltpu.make_async_copy(wq_hbm.at[:, pl.ds(col, 128)], wkq.at[:, pl.ds(128, 128)], lsem.at[1]),
        pltpu.make_async_copy(wv_hbm, wv, lsem.at[2]),
        pltpu.make_async_copy(ek_hbm, ek, lsem.at[3]),
        pltpu.make_async_copy(eq_hbm, eq, lsem.at[4]),
        pltpu.make_async_copy(sel_hbm, sel, lsem.at[5]),
    ]
    loads[0].start()
    loads[1].start()
    hid_copy(lax.rem(y + 1, ny)).start()
    loads[2].start()
    loads[3].start()
    for s in range(1, ny):
        hid_copy(lax.rem(y + 1 + s, ny)).start()
    loads[4].start()
    loads[5].start()

    barrier = pltpu.get_barrier_semaphore()
    peers = [(z, y, other, x)]
    peers += [(z, lax.rem(y + d, ny), c, x) for d in range(1, ny)]
    peers += [(lax.rem(z + d, nz), y, c, x) for d in range(1, nz)]
    peers += [(z, y, c, lax.rem(x + d, nx)) for d in range(1, nx)]
    for peer in peers:
        pl.semaphore_signal(barrier, inc=1, device_id=peer, device_id_type=MESH)
    pl.semaphore_wait(barrier, len(peers))

    def remote(src, dst, send, recv, dev):
        return pltpu.make_async_remote_copy(
            src_ref=src, dst_ref=dst, send_sem=send, recv_sem=recv, device_id=dev, device_id_type=MESH
        )

    core = (z, y, other, x)

    def at_y(q):
        return (z, q, c, x)

    def at_z(q):
        return (q, y, c, x)

    def at_x(q):
        return (z, y, c, q)

    for load in loads[:4]:
        load.wait()
    ones = jnp.ones((8, span), BF16)

    def to_core(p):
        return remote(loc.at[p, other], r0.at[p], s0.at[p], v0.at[p], core)

    def chip_sum(p):
        to_core(p).wait_recv()
        csum[p] = (loc[p, c].astype(F32) + r0[p].astype(F32)).astype(BF16)

    def sum_to_y(p):
        return remote(csum.at[p], ry.at[y], sy.at[p], vy.at[y], at_y(p))

    def state(s, carry):
        p = lax.rem(y + 1 + s, ny)
        hid_copy(p).wait()
        rows = hid[p]
        kq = dot(rows, wkq[...])
        k = pltpu.roll(kq[:, :128], shift, 1).astype(BF16).astype(F32)
        q = pltpu.roll(kq[:, 128:], shift, 1)
        lane = lax.broadcasted_iota(jnp.int32, (span, 128), 1)
        qry[p] = jnp.where(lane < 64, q, jnp.where(lane == 65, 1.0, 0.0)).astype(BF16)
        kt = jnp.transpose(k)
        row = lax.broadcasted_iota(jnp.int32, (128, span), 0)
        live = (lax.broadcasted_iota(jnp.int32, (128, span), 1) + pos0 < len_ref[p]).astype(F32)
        kt = jnp.where(row < 64, kt, jnp.where(row == 64, 1.0, 0.0)) * live + jnp.where(row == 65, 1.0, 0.0)
        kt = kt.astype(BF16)
        keyt[p] = kt
        val[p] = dot(rows, wv[...]).astype(BF16)
        for h in range(HL):
            left = dot(ek[h * ROWS : (h + 1) * ROWS], kt)
            right = dot(ek[(HL + h) * ROWS : (HL + h + 1) * ROWS], kt)
            feat = (left * right).astype(BF16)
            st = dot(feat, val[p, :, h * HD : (h + 1) * HD])
            zn = dot(ones, feat, 1, 1)
            first = zn[:, :128]
            rest = jnp.concatenate([zn[:, 128:], jnp.zeros((8, 256 - ROWS), F32)], axis=1)
            sub = lax.broadcasted_iota(jnp.int32, (8, 128), 0)
            tail = jnp.where(sub == 1, first, jnp.where(sub == 2, rest, st[ROWS - 8 :]))
            loc[p, h // 2, h % 2] = jnp.concatenate([st[: ROWS - 8], tail], axis=0).astype(BF16)
        to_core(p).start()

        @pl.when(s > 0)
        def _():
            before = lax.rem(y + s, ny)
            chip_sum(before)
            sum_to_y(before).start()

        return carry

    lax.fori_loop(0, ny, state, 0)

    chip_sum(y)
    ry[y] = csum[y]
    for d in range(1, ny):
        q = lax.rem(y + d, ny)
        remote(csum.at[q], ry.at[q], sy.at[q], vy.at[q], at_y(q)).wait_recv()
    total = ry[0].astype(F32)
    for q in range(1, ny):
        total = total + ry[q].astype(F32)
    total = total.reshape(2 * ROWS, HD)
    for q in range(nz):
        tz[q] = total[q * zr : (q + 1) * zr].astype(BF16)

    def slice_to_z(q):
        return remote(tz.at[q], rz.at[z], sz.at[q], vz.at[z], at_z(q))

    for d in range(1, nz):
        slice_to_z(lax.rem(z + d, nz)).start()
    rz[z] = tz[z]

    for load in loads[4:]:
        load.wait()

    def inside(p):
        q = qry[p]
        t_at = lax.broadcasted_iota(jnp.int32, (span, span), 0)
        u_at = lax.broadcasted_iota(jnp.int32, (span, span), 1)
        seen = (u_at <= t_at) & (u_at + pos0 < len_ref[p])
        row = lax.broadcasted_iota(jnp.int32, (128, span), 0)
        kt = keyt[p]
        for h in range(HL):
            phi[p, h] = (dot(q, eq[h]) * dot(q, eq[HL + h])).astype(BF16)
            mine = jnp.where((row >= h * FD) & (row < (h + 1) * FD), kt, jnp.zeros_like(kt))
            half = dot(q, mine) * 0.25 + 1.0
            weight = jnp.where(seen, half * half * 0.5 + 0.5, 0.0).astype(BF16)
            nself[p, h] = dot(weight, val[p, :, h * HD : (h + 1) * HD])
            dself[p, h] = dot(weight, jnp.ones((span, HD), BF16))

    def inside_step(p, carry):
        inside(p)
        return carry

    lax.fori_loop(0, ny // 2, inside_step, 0)

    for d in range(1, nz):
        q = lax.rem(z + d, nz)
        remote(tz.at[q], rz.at[q], sz.at[q], vz.at[q], at_z(q)).wait_recv()
    run = jnp.zeros((zr, HD), F32)
    for q in range(nz):
        pz[q] = run.astype(BF16)
        run = run + rz[q].astype(F32)
    tt[...] = run.astype(BF16)

    def prefix_to_z(q):
        return remote(pz.at[q], rpz.at[z], sz2.at[q], vz2.at[z], at_z(q))

    def total_to_z(q):
        return remote(tt, rtt.at[z], sz3.at[q], vz3.at[z], at_z(q))

    for d in range(1, nz):
        prefix_to_z(lax.rem(z + d, nz)).start()
    rpz[z] = pz[z]
    for d in range(1, nz):
        total_to_z(lax.rem(z + d, nz)).start()
    rtt[z] = tt[...]

    lax.fori_loop(ny // 2, ny, inside_step, 0)

    for d in range(1, nz):
        q = lax.rem(z + d, nz)
        remote(pz.at[q], rpz.at[q], sz2.at[q], vz2.at[q], at_z(q)).wait_recv()
    run = jnp.concatenate([rpz[q].astype(F32) for q in range(nz)], axis=0).reshape(2, ROWS, HD)
    for q in range(ny):
        py[q] = run.astype(BF16)
        run = run + ry[q].astype(F32)

    def prefix_to_y(q):
        return remote(py.at[q], rpy.at[y], sy2.at[q], vy2.at[y], at_y(q))

    for d in range(1, ny):
        prefix_to_y(lax.rem(y + d, ny)).start()
    rpy[y] = py[y]

    part = sel.shape[0] // nx
    for d in range(1, nz):
        q = lax.rem(z + d, nz)
        remote(tt, rtt.at[q], sz3.at[q], vz3.at[q], at_z(q)).wait_recv()
    whole = jnp.concatenate([rtt[q].astype(F32) for q in range(nz)], axis=0).reshape(2, ROWS, HD).astype(BF16)
    for i in range(2):
        picked = dot(sel[...], whole[i]).astype(BF16)
        for q in range(nx):
            fxs[q, i] = picked[q * part : (q + 1) * part]
        lowa[c, y, i] = whole[i, 128:]

    def final_to_x(q):
        return remote(fxs.at[q], fxa.at[c, y, x], sx.at[q], vx.at[x], at_x(q))

    for d in range(1, nx):
        final_to_x(lax.rem(x + d, nx)).start()
    fxa[c, y, x] = fxs[x]

    def attend(p, h, state):
        tail = state[ROWS - 8 :]
        norm = jnp.concatenate(
            [jnp.broadcast_to(tail[1:2], (HD, HD)), jnp.broadcast_to(tail[2:3, : ROWS - HD], (HD, ROWS - HD))], axis=1
        ).astype(BF16)
        feats = phi[p, h]
        num = dot(feats, state.astype(BF16)) + nself[p, h]
        den = dot(feats, norm, 1, 1) + dself[p, h]
        live = lax.broadcasted_iota(jnp.int32, (span, HD), 0) + pos0 < len_ref[p]
        att[p, h] = jnp.where(live, num / den, 0.0)

    def to_core2(p):
        return remote(pc.at[p], rpc.at[p], s02.at[p], v02.at[p], core)

    at_one = (c == 1).astype(F32)

    def near(s, carry):
        p = lax.rem(y + s, ny)

        @pl.when(s > 0)
        def _():
            remote(py.at[p], rpy.at[p], sy2.at[p], vy2.at[p], at_y(p)).wait_recv()

        chip = rpy[p].astype(F32)
        pc[p] = (chip + (1.0 - at_one) * loc[p, c].astype(F32)).astype(BF16)
        to_core2(p).start()
        mine = chip + at_one * r0[p].astype(F32)
        for i in range(2):
            attend(p, c * 2 + i, mine[i])
        return carry

    lax.fori_loop(0, ny, near, 0)

    for d in range(1, nx):
        q = lax.rem(x + d, nx)
        remote(fxs.at[q], fxa.at[c, y, q], sx.at[q], vx.at[q], at_x(q)).wait_recv()

    def final_to_y(q):
        return remote(fxa.at[c, y], fxa.at[c, y], sy3.at[q], vy3.at[y], at_y(q))

    def low_to_y(q):
        return remote(lowa.at[c, y], lowa.at[c, y], sy4.at[q], vy4.at[y], at_y(q))

    for d in range(1, ny):
        q = lax.rem(y + d, ny)
        final_to_y(q).start()
        low_to_y(q).start()

    def far(s, carry):
        p = lax.rem(y + s, ny)
        to_core2(p).wait_recv()
        there = rpc[p].astype(F32)
        for i in range(2):
            attend(p, other * 2 + i, there[i])
        square = att[p, 0] * att[p, 0]
        for h in range(1, HL):
            square = square + att[p, h] * att[p, h]
        high = square.astype(BF16)
        rest = (square - high.astype(F32)).astype(BF16)
        unit = jnp.ones((8, HD), BF16)
        sq[p] = dot(unit, high, 1, 1) + dot(unit, rest, 1, 1)
        return carry

    lax.fori_loop(0, ny, far, 0)

    def square_to_x(q):
        return remote(sq, rsq.at[x], sx2.at[q], vx2.at[x], at_x(q))

    for d in range(1, nx):
        square_to_x(lax.rem(x + d, nx)).start()

    for d in range(1, ny):
        q = lax.rem(y + d, ny)
        remote(fxa.at[c, y], fxa.at[c, q], sy3.at[q], vy3.at[q], at_y(q)).wait_recv()
        remote(lowa.at[c, y], lowa.at[c, q], sy4.at[q], vy4.at[q], at_y(q)).wait_recv()
    final_to_core = remote(fxa.at[c], fxa.at[c], s3.at[0], v3.at[0], core)
    low_to_core = remote(lowa.at[c], lowa.at[c], s3.at[1], v3.at[1], core)
    final_to_core.start()
    low_to_core.start()

    rsq[x] = sq[...]
    for d in range(1, nx):
        q = lax.rem(x + d, nx)
        remote(sq, rsq.at[q], sx2.at[q], vx2.at[q], at_x(q)).wait_recv()

    def out_copy(p):
        return pltpu.make_async_copy(mixed.at[p], mixed_hbm.at[p], osem.at[p])

    def scale(p, carry):
        squares = rsq[0, p]
        for q in range(1, nx):
            squares = squares + rsq[q, p]
        factor = lax.rsqrt(squares / width + NORM_FLOOR)
        cm[...] = jnp.transpose(factor)
        factor = jnp.broadcast_to(cm[:, 0:1], (span, HD))
        for h in range(HL):
            mixed[p, :, h * HD : (h + 1) * HD] = (att[p, h] * factor).astype(BF16)
        out_copy(p).start()
        return carry

    lax.fori_loop(0, ny, scale, 0)

    remote(fxa.at[c], fxa.at[other], s3.at[0], v3.at[0], core).wait_recv()
    remote(lowa.at[c], lowa.at[other], s3.at[1], v3.at[1], core).wait_recv()
    outs = [
        pltpu.make_async_copy(fxa, fx_hbm, osem.at[ny]),
        pltpu.make_async_copy(lowa, low_hbm, osem.at[ny + 1]),
    ]
    for out in outs:
        out.start()

    for p in range(ny):
        to_core(p).wait_send()
        to_core2(p).wait_send()
    for d in range(1, ny):
        q = lax.rem(y + d, ny)
        sum_to_y(q).wait_send()
        prefix_to_y(q).wait_send()
        final_to_y(q).wait_send()
        low_to_y(q).wait_send()
    for d in range(1, nz):
        q = lax.rem(z + d, nz)
        slice_to_z(q).wait_send()
        prefix_to_z(q).wait_send()
        total_to_z(q).wait_send()
    for d in range(1, nx):
        q = lax.rem(x + d, nx)
        final_to_x(q).wait_send()
        square_to_x(q).wait_send()
    final_to_core.wait_send()
    low_to_core.wait_send()
    for p in range(ny):
        out_copy(p).wait()
    for out in outs:
        out.wait()


def body(hidden_in, w_query, w_key, w_value, lengths, owners):
    nz, ny, nc, nx = (lax.axis_size(a) for a in ("z", "y", "c", "x"))
    prompts, span, width = hidden_in.shape
    own = FD // nx * FD
    part = own + 16
    zr = 2 * ROWS // nz
    ek, eq, sel = (jnp.asarray(t) for t in tables(nx))
    anyspace = pl.BlockSpec(memory_space=pl.ANY)
    dma = pltpu.SemaphoreType.DMA

    def vmem(*shape, kind=BF16):
        return pltpu.VMEM(shape, kind)

    block = (2, ROWS, HD)
    mixed, fx, low = pl.pallas_call(
        functools.partial(kernel, (nz, ny, nc, nx, span, HD * HL * nx)),
        out_shape=(
            jax.ShapeDtypeStruct((prompts, span, HL * HD), BF16),
            jax.ShapeDtypeStruct((nc, prompts, nx, 2, part, HD), BF16),
            jax.ShapeDtypeStruct((nc, prompts, 2, ROWS - 128, HD), BF16),
        ),
        in_specs=[pl.BlockSpec(memory_space=pltpu.SMEM)] + [anyspace] * 7,
        out_specs=(anyspace,) * 3,
        scratch_shapes=[
            vmem(prompts, span, width), vmem(width, HL * HD), vmem(width, 256),
            vmem(*ek.shape), vmem(*eq.shape), vmem(*sel.shape),
            vmem(prompts, span, HL * HD), vmem(prompts, 128, span), vmem(prompts, span, 128),
            vmem(prompts, HL, span, ROWS),
            vmem(prompts, HL, span, HD, kind=F32), vmem(prompts, HL, span, HD, kind=F32),
            vmem(prompts, HL, span, HD, kind=F32),
            vmem(prompts, span, HL * HD), vmem(span, 8, kind=F32),
            vmem(prompts, 8, span, kind=F32), vmem(nx, prompts, 8, span, kind=F32),
            vmem(prompts, 2, *block), vmem(prompts, *block), vmem(prompts, *block), vmem(ny, *block),
            vmem(nz, zr, HD), vmem(nz, zr, HD), vmem(nz, zr, HD), vmem(nz, zr, HD), vmem(zr, HD), vmem(nz, zr, HD),
            vmem(ny, *block), vmem(prompts, *block), vmem(prompts, *block), vmem(prompts, *block),
            vmem(nx, 2, part, HD), vmem(nc, prompts, nx, 2, part, HD), vmem(nc, prompts, 2, ROWS - 128, HD),
            dma((6,)), dma((prompts,)), dma((prompts,)), dma((prompts,)),
            dma((ny,)), dma((ny,)), dma((nz,)), dma((nz,)), dma((nz,)), dma((nz,)), dma((nz,)), dma((nz,)),
            dma((ny,)), dma((ny,)), dma((prompts,)), dma((prompts,)),
            dma((nx,)), dma((nx,)), dma((ny,)), dma((ny,)), dma((ny,)), dma((ny,)), dma((2,)), dma((2,)),
            dma((nx,)), dma((nx,)), dma((prompts + 2,)),
        ],
        compiler_params=pltpu.CompilerParams(
            collective_id=0, has_side_effects=True, vmem_limit_bytes=60 * 1024 * 1024
        ),
        name="prefill",
    )(lengths, hidden_in, w_value, w_key, w_query, ek, eq, sel)

    owned = owners == lax.axis_index(SEQ)
    fx = jnp.transpose(fx, (1, 2, 0, 3, 4, 5)).reshape(prompts, HL * nx, part, HD)
    low = jnp.transpose(low, (1, 0, 2, 3, 4)).reshape(prompts, HL, ROWS - 128, HD)
    quad_scale = (2.0 * FD) ** (-0.5)
    low_scale = FD ** (-0.25)
    state_quad = jnp.where(owned[:, None, None, None], fx[:, :, :own].astype(F32) * quad_scale, 0.0)[None]
    norms = jnp.concatenate([fx[:, :, own], fx[:, :, own + 1, : ROWS - 128]], axis=-1)
    pick = lax.dynamic_slice_in_dim(sel, lax.axis_index("x") * part, own, 0)
    norm_quad = dot(norms.reshape(prompts * HL * nx, ROWS), pick, 1, 1).reshape(prompts, HL * nx, own)
    norm_quad = jnp.where(owned[:, None, None], norm_quad * quad_scale, 0.0)[None]
    lin, one = LIN - 128, ONE - 128
    state_low = jnp.concatenate(
        [low[:, :, one : one + 1].astype(F32), low[:, :, lin : lin + FD].astype(F32) * low_scale], axis=2
    )
    state_low = jnp.where(owned[:, None, None, None], state_low, 0.0)[None]
    rest = low[:, :, NORM + 1 - 128].astype(F32)
    norm_low = jnp.concatenate([rest[..., one : one + 1], rest[..., lin : lin + FD] * low_scale], axis=-1)
    norm_low = jnp.where(owned[:, None, None], norm_low, 0.0)[None]
    return mixed, state_quad, state_low, norm_quad, norm_low


def torus_of(mesh, shape=(8, 4, 2, 4)):
    return Mesh(mesh.devices.reshape(shape), ("z", "y", "c", "x"))


def run_on(torus):
    return jax.shard_map(
        body,
        mesh=torus,
        in_specs=(P(None, SEQ, None), P(), P(), P(None, "x"), P(), P()),
        out_specs=(
            P(None, SEQ, "x"),
            P(SEQ, None, None, "x", None),
            P(SEQ, None, "x", None, None),
            P(SEQ, None, None, "x"),
            P(SEQ, None, "x", None),
        ),
        check_vma=False,
    )


def solution(mesh):
    ny, nc = 4, 2
    feat = mesh.shape["feat"]
    return run_on(torus_of(mesh, (mesh.shape["seq"] // (ny * nc), ny, nc, feat)))
```

```python
import functools

import jax
import jax.numpy as jnp
import numpy as np
from jax import lax
from jax.experimental import pallas as pl
from jax.experimental.pallas import tpu as pltpu
from jax.sharding import Mesh
from jax.sharding import PartitionSpec as P

MESH = pl.DeviceIdType.MESH
F32, BF16 = jnp.float32, jnp.bfloat16
FD = 16
ROWS = 160
LIN, ONE, NORM = 136, 152, 153
HD = 128
NORM_FLOOR = 0.0001
HL = 4
SEQ = ("z", "y", "c")


def packed_pairs():
    pairs = [(i, (i + d) % FD, d) for d in range(8) for i in range(FD)]
    return pairs + [(i, i + 8, 8) for i in range(8)]


def row_of(i, j):
    d = (j - i) % FD
    if d < 8:
        return d * FD + i
    if d == 8:
        return 8 * FD + min(i, j)
    return (FD - d) * FD + j


@functools.cache
def tables(nx):
    eq = np.zeros((2, HL, 128, ROWS), np.float32)
    for h in range(HL):
        for r, (i, j, d) in enumerate(packed_pairs()):
            eq[0, h, h * FD + i, r] = 1.0 / 32 if d == 0 else 1.0 / 16
            eq[1, h, h * FD + j, r] = 1.0
        for i in range(FD):
            eq[0, h, h * FD + i, LIN + i] = 0.25
            eq[1, h, 65, LIN + i] = 1.0
        eq[0, h, 65, ONE] = eq[1, h, 65, ONE] = 1.0
    own = FD // nx
    sel = np.zeros((nx, own * FD, ROWS), np.float32)
    for x in range(nx):
        for ii in range(own):
            for j in range(FD):
                sel[x, ii * FD + j, row_of(x * own + ii, j)] = 1.0
    return (
        eq.reshape(2 * HL, 128, ROWS).astype(BF16),
        sel.reshape(-1, ROWS).astype(BF16),
    )


def dot(a, b, ca=1, cb=0):
    return lax.dot_general(a, b, (((ca,), (cb,)), ((), ())), preferred_element_type=F32)


def kernel(
    sizes, len_ref, hid_hbm, wv_hbm, wk_hbm, wq_hbm, eq_hbm, sel_hbm, mixed_hbm, fx_hbm, low_hbm,
    hid, wv, wk, wkt, wq, eq, sel, val, keyt, kd, phi, nself, dself, att, mixed, sq, rsq,
    loc, r0, csum, ry, tz, rz, pz, rpz, tt, rtt, py, rpy, pc, rpc, fxs, fxa, lowa,
    lsem, hsem, s0, v0, sy, vy, sz, vz, sz2, vz2, sz3, vz3, sy2, vy2, s02, v02,
    sx, vx, sy3, vy3, sy4, vy4, s3, v3, s4, v4, sx2, vx2, osem,
):
    nz, ny, nc, nx, span, width = sizes
    width_in = wk.shape[0]
    zr = 2 * ROWS // nz
    z, y, c, x = (lax.axis_index(a) for a in ("z", "y", "c", "x"))
    other = 1 - c
    pos0 = ((z * ny + y) * nc + c) * span

    col = pl.multiple_of((x * (HL * FD)) // 128 * 128, 128)
    shift = lax.rem(x * (HL * FD), 128)

    def turn(s):
        return lax.rem(y + jnp.where(s == 0, 2, jnp.where(s == 1, 1, jnp.where(s == 2, 3, 0))), ny)

    def hid_copy(p):
        return pltpu.make_async_copy(hid_hbm.at[p], hid.at[p], hsem.at[p])

    loads = [
        pltpu.make_async_copy(wk_hbm.at[:, pl.ds(col, 128)], wk, lsem.at[0]),
        pltpu.make_async_copy(wv_hbm, wv, lsem.at[1]),
        pltpu.make_async_copy(wq_hbm.at[:, pl.ds(col, 128)], wq, lsem.at[2]),
        pltpu.make_async_copy(eq_hbm, eq, lsem.at[3]),
        pltpu.make_async_copy(sel_hbm, sel, lsem.at[4]),
    ]
    loads[0].start()
    hid_copy(turn(0)).start()
    loads[1].start()
    for s in range(1, ny):
        hid_copy(turn(s)).start()
    for load in loads[2:]:
        load.start()

    barrier = pltpu.get_barrier_semaphore()
    peers = [(z, y, other, x)]
    peers += [(z, lax.rem(y + d, ny), c, x) for d in range(1, ny)]
    peers += [(lax.rem(z + d, nz), y, c, x) for d in range(1, nz)]
    peers += [(z, y, c, lax.rem(x + d, nx)) for d in range(1, nx)]
    for peer in peers:
        pl.semaphore_signal(barrier, inc=1, device_id=peer, device_id_type=MESH)

    def remote(src, dst, send, recv, dev):
        return pltpu.make_async_remote_copy(
            src_ref=src, dst_ref=dst, send_sem=send, recv_sem=recv, device_id=dev, device_id_type=MESH
        )

    core = (z, y, other, x)

    def at_y(q):
        return (z, q, c, x)

    def at_z(q):
        return (q, y, c, x)

    def at_x(q):
        return (z, y, c, q)

    loads[0].wait()
    for r in range(0, width_in, 256):
        wkt[:, r : r + 256] = jnp.transpose(wk[r : r + 256])
    keyt[...] = jnp.zeros(keyt.shape, BF16)
    far_z = sorted(range(1, nz), key=lambda d: -min(d, nz - d))
    far_y = [d for d in (1, 3, 2) if d < ny]
    ones = jnp.ones((8, span), BF16)
    sq[...] = jnp.zeros(sq.shape, F32)

    def to_core(p):
        return remote(loc.at[p, other], r0.at[p], s0.at[p], v0.at[p], core)

    def chip_sum(p):
        to_core(p).wait_recv()
        csum[p] = (loc[p, c].astype(F32) + r0[p].astype(F32)).astype(BF16)

    def sum_to_y(p):
        return remote(csum.at[p], ry.at[y], sy.at[p], vy.at[y], at_y(p))

    def state(s, carry):
        p = turn(s)
        hid_copy(p).wait()
        kt = dot(wkt[pl.ds(pl.multiple_of(shift, 64), HL * FD)], hid[p], 1, 1).astype(BF16).astype(F32)
        live = (lax.broadcasted_iota(jnp.int32, (HL * FD, span), 1) + pos0 < len_ref[p]).astype(F32)
        kt = kt * live
        keyt[p, : HL * FD] = kt.astype(BF16)
        for h in range(HL):
            for t in range(span // 128):
                piece = kt[h * FD : (h + 1) * FD, t * 128 : (t + 1) * 128]
                kd[t, h, :FD] = piece
                kd[t, h, FD:] = piece

        @pl.when(s == 0)
        def _():
            loads[1].wait()

        val[p] = dot(hid[p], wv[...]).astype(BF16)

        @pl.when(s == 0)
        def _():
            pl.semaphore_wait(barrier, len(peers))

        @pl.when(s > 0)
        def _():
            before = turn(s - 1)
            chip_sum(before)
            sum_to_y(before).start()

        sub = lax.broadcasted_iota(jnp.int32, (8, 128), 0)
        for n in range(HL):
            pair = other if n < 2 else c
            h = pair * 2 + n % 2
            halves = []
            for t in range(span // 128):
                mine = kd[t, h, :FD]
                rows = [mine * kd[t, h, d : d + FD] for d in range(8)]
                rows += [mine[:8] * mine[8:], mine]
                rows += [jnp.where(sub == 0, live[:8, t * 128 : (t + 1) * 128], 0.0)]
                halves.append(jnp.concatenate(rows, axis=0).astype(BF16))
            feat = jnp.concatenate(halves, axis=1)
            st = dot(feat, val[p, :, pl.ds(pl.multiple_of(h * HD, HD), HD)])
            zn = dot(ones, feat, 1, 1)
            first = zn[:, :128]
            rest = jnp.concatenate([zn[:, 128:], jnp.zeros((8, 256 - ROWS), F32)], axis=1)
            tail = jnp.where(sub == 1, first, jnp.where(sub == 2, rest, st[ROWS - 8 :]))
            loc[p, pair, n % 2] = jnp.concatenate([st[: ROWS - 8], tail], axis=0).astype(BF16)
            if n == 1:
                to_core(p).start()
        return carry

    lax.fori_loop(0, ny, state, 0)

    chip_sum(y)
    ry[y] = csum[y]
    for d in range(1, ny):
        q = lax.rem(y + d, ny)
        remote(csum.at[q], ry.at[q], sy.at[q], vy.at[q], at_y(q)).wait_recv()
    total = ry[0].astype(F32)
    for q in range(1, ny):
        total = total + ry[q].astype(F32)
    total = total.reshape(2 * ROWS, HD)
    for q in range(nz):
        tz[q] = total[q * zr : (q + 1) * zr].astype(BF16)

    def slice_to_z(q):
        return remote(tz.at[q], rz.at[z], sz.at[q], vz.at[z], at_z(q))

    for d in far_z:
        slice_to_z(lax.rem(z + d, nz)).start()
    rz[z] = tz[z]

    for load in loads[2:]:
        load.wait()

    def inside(p):
        q = pltpu.roll(dot(hid[p], wq[...]), shift, 1)
        lane = lax.broadcasted_iota(jnp.int32, (span, 128), 1)
        q = jnp.where(lane < HL * FD, q, jnp.where(lane == 65, 1.0, 0.0)).astype(BF16)
        t_at = lax.broadcasted_iota(jnp.int32, (span, span), 0)
        u_at = lax.broadcasted_iota(jnp.int32, (span, span), 1)
        seen = (u_at <= t_at) & (u_at + pos0 < len_ref[p])
        row = lax.broadcasted_iota(jnp.int32, (128, span), 0)
        kt = keyt[p]
        for h in range(HL):
            phi[p, h] = (dot(q, eq[h]) * dot(q, eq[HL + h])).astype(BF16)
            mine = jnp.where((row >= h * FD) & (row < (h + 1) * FD), kt, jnp.zeros_like(kt))
            half = dot(q, mine) * 0.25 + 1.0
            weight = jnp.where(seen, half * half * 0.5 + 0.5, 0.0).astype(BF16)
            nself[p, h] = dot(weight, val[p, :, h * HD : (h + 1) * HD])
            dself[p, h] = dot(weight, jnp.ones((span, HD), BF16))

    def inside_step(p, carry):
        inside(p)
        return carry

    lax.fori_loop(0, ny // 2, inside_step, 0)

    for d in range(1, nz):
        q = lax.rem(z + d, nz)
        remote(tz.at[q], rz.at[q], sz.at[q], vz.at[q], at_z(q)).wait_recv()
    run = jnp.zeros((zr, HD), F32)
    for q in range(nz):
        pz[q] = run.astype(BF16)
        run = run + rz[q].astype(F32)
    tt[...] = run.astype(BF16)

    def prefix_to_z(q):
        return remote(pz.at[q], rpz.at[z], sz2.at[q], vz2.at[z], at_z(q))

    def total_to_z(q):
        return remote(tt, rtt.at[z], sz3.at[q], vz3.at[z], at_z(q))

    for d in far_z:
        prefix_to_z(lax.rem(z + d, nz)).start()
    rpz[z] = pz[z]
    for d in far_z:
        total_to_z(lax.rem(z + d, nz)).start()
    rtt[z] = tt[...]

    lax.fori_loop(ny // 2, ny, inside_step, 0)

    for d in range(1, nz):
        q = lax.rem(z + d, nz)
        remote(pz.at[q], rpz.at[q], sz2.at[q], vz2.at[q], at_z(q)).wait_recv()
    run = jnp.concatenate([rpz[q].astype(F32) for q in range(nz)], axis=0).reshape(2, ROWS, HD)
    for q in range(ny):
        py[q] = run.astype(BF16)
        run = run + ry[q].astype(F32)

    def prefix_to_y(q):
        return remote(py.at[q], rpy.at[y], sy2.at[q], vy2.at[y], at_y(q))

    for d in far_y:
        prefix_to_y(lax.rem(y + d, ny)).start()
    rpy[y] = py[y]

    own = sel.shape[0] // nx
    for d in range(1, nz):
        q = lax.rem(z + d, nz)
        remote(tt, rtt.at[q], sz3.at[q], vz3.at[q], at_z(q)).wait_recv()
    whole = jnp.concatenate([rtt[q].astype(F32) for q in range(nz)], axis=0).reshape(2, ROWS, HD)
    tails = jnp.concatenate([whole[0, ROWS - 8 :], whole[1, ROWS - 8 :]], axis=0).astype(BF16)
    whole = whole.astype(BF16)
    for i in range(2):
        picked = dot(sel[...], whole[i]).astype(BF16)
        for q in range(nx):
            fxs[q, i * own : (i + 1) * own] = picked[q * own : (q + 1) * own]
        lowa[y, i] = whole[i, 128:]
    for q in range(nx):
        fxs[q, 2 * own :] = tails

    def final_to_x(q):
        return remote(fxs.at[q], fxa.at[y, x], sx.at[q], vx.at[x], at_x(q))

    for d in range(1, nx):
        final_to_x(lax.rem(x + d, nx)).start()
    fxa[y, x] = fxs[x]


    def attend(p, h, state):
        tail = state[ROWS - 8 :]
        norm = jnp.concatenate(
            [jnp.broadcast_to(tail[1:2], (HD, HD)), jnp.broadcast_to(tail[2:3, : ROWS - HD], (HD, ROWS - HD))], axis=1
        ).astype(BF16)
        feats = phi[p, h]
        num = dot(feats, state.astype(BF16)) + nself[p, h]
        den = dot(feats, norm, 1, 1) + dself[p, h]
        live = lax.broadcasted_iota(jnp.int32, (span, HD), 0) + pos0 < len_ref[p]
        att[p, h] = jnp.where(live, num / den, 0.0)

    def to_core2(p):
        return remote(pc.at[p], rpc.at[p], s02.at[p], v02.at[p], core)

    at_one = (c == 1).astype(F32)

    def near(p):
        chip = rpy[p].astype(F32)
        pc[p] = (chip + (1.0 - at_one) * loc[p, c].astype(F32)).astype(BF16)
        to_core2(p).start()
        mine = chip + at_one * r0[p].astype(F32)
        for i in range(2):
            attend(p, c * 2 + i, mine[i])

    def far(p):
        to_core2(p).wait_recv()
        there = rpc[p].astype(F32)
        for i in range(2):
            attend(p, other * 2 + i, there[i])
        square = att[p, 0] * att[p, 0]
        for h in range(1, HL):
            square = square + att[p, h] * att[p, h]
        high = square.astype(BF16)
        rest = (square - high.astype(F32)).astype(BF16)
        unit = jnp.ones((8, HD), BF16)
        sq[pl.ds(p, 1)] = (dot(unit, high, 1, 1) + dot(unit, rest, 1, 1))[0:1]

    def final_to_core(p):
        return remote(fxa.at[p], fx_hbm.at[c, p], s3.at[p], v3.at[p], core)

    def low_to_core(p):
        return remote(lowa.at[p], low_hbm.at[c, p], s4.at[p], v4.at[p], core)

    def final_here(p):
        return pltpu.make_async_copy(fxa.at[p], fx_hbm.at[c, p], osem.at[ny + p])

    def low_here(p):
        return pltpu.make_async_copy(lowa.at[p], low_hbm.at[c, p], osem.at[2 * ny + p])

    def deliver(p):
        for copy in (final_to_core(p), low_to_core(p), final_here(p), low_here(p)):
            copy.start()

    def turn_back(s):
        return lax.rem(y + jnp.where(s == 0, 3, s), ny)

    def near_step(s, carry):
        p = turn_back(s)
        remote(py.at[p], rpy.at[p], sy2.at[p], vy2.at[p], at_y(p)).wait_recv()
        near(p)
        return carry

    def far_step(s, carry):
        far(turn_back(s))
        return carry

    near(y)
    lax.fori_loop(0, ny - 1, near_step, 0)
    far(y)

    for d in range(1, nx):
        q = lax.rem(x + d, nx)
        remote(fxs.at[q], fxa.at[y, q], sx.at[q], vx.at[q], at_x(q)).wait_recv()

    def final_to_y(q):
        return remote(fxa.at[y], fxa.at[y], sy3.at[q], vy3.at[y], at_y(q))

    def low_to_y(q):
        return remote(lowa.at[y], lowa.at[y], sy4.at[q], vy4.at[y], at_y(q))

    for d in far_y:
        q = lax.rem(y + d, ny)
        final_to_y(q).start()
        low_to_y(q).start()

    deliver(y)
    lax.fori_loop(0, ny - 1, far_step, 0)

    def square_to_x(q):
        return remote(sq, rsq.at[x], sx2.at[q], vx2.at[x], at_x(q))

    for d in range(1, nx):
        square_to_x(lax.rem(x + d, nx)).start()

    rsq[x] = sq[...]
    for d in range(1, nx):
        q = lax.rem(x + d, nx)
        remote(sq, rsq.at[q], sx2.at[q], vx2.at[q], at_x(q)).wait_recv()

    def mixed_out(p):
        return pltpu.make_async_copy(mixed.at[p], mixed_hbm.at[p], osem.at[p])

    squares = rsq[0]
    for q in range(1, nx):
        squares = squares + rsq[q]
    factor = jnp.transpose(lax.rsqrt(squares / width + NORM_FLOOR))
    for p in range(ny):
        scale = jnp.broadcast_to(factor[:, p : p + 1], (span, HD))
        for h in range(HL):
            mixed[p, :, h * HD : (h + 1) * HD] = (att[p, h] * scale).astype(BF16)
        mixed_out(p).start()

    for s in (3, 1, 2):
        q = lax.rem(y + s, ny)
        remote(fxa.at[y], fxa.at[q], sy3.at[q], vy3.at[q], at_y(q)).wait_recv()
        remote(lowa.at[y], lowa.at[q], sy4.at[q], vy4.at[q], at_y(q)).wait_recv()
        deliver(q)

    for p in range(ny):
        remote(fxa.at[p], fx_hbm.at[other, p], s3.at[p], v3.at[p], core).wait_recv()
        remote(lowa.at[p], low_hbm.at[other, p], s4.at[p], v4.at[p], core).wait_recv()

    for p in range(ny):
        to_core(p).wait_send()
        to_core2(p).wait_send()
    for d in range(1, ny):
        q = lax.rem(y + d, ny)
        sum_to_y(q).wait_send()
        prefix_to_y(q).wait_send()
        final_to_y(q).wait_send()
        low_to_y(q).wait_send()
    for d in range(1, nz):
        q = lax.rem(z + d, nz)
        slice_to_z(q).wait_send()
        prefix_to_z(q).wait_send()
        total_to_z(q).wait_send()
    for d in range(1, nx):
        q = lax.rem(x + d, nx)
        final_to_x(q).wait_send()
        square_to_x(q).wait_send()
    for p in range(ny):
        final_to_core(p).wait_send()
        low_to_core(p).wait_send()
        final_here(p).wait()
        low_here(p).wait()
        mixed_out(p).wait()


def finish(
    sizes, own_ref, scaled_hbm, fx_hbm, low_hbm, sel_hbm, mixed_hbm, quad_hbm, slow_hbm, nquad_hbm, nlow_hbm,
    fx, low, sel, mixed, quad, slow, nquad, nlow, isem, osem,
):
    nz, ny, nc, nx, prompts = sizes
    z, y, c, x = (lax.axis_index(a) for a in ("z", "y", "c", "x"))
    here = (z * ny + y) * nc + c
    own = sel.shape[0]

    def mixed_in(p):
        return pltpu.make_async_copy(scaled_hbm.at[p], mixed.at[p], isem.at[p])

    def fx_in(p):
        return pltpu.make_async_copy(fx_hbm.at[:, p], fx.at[:, p], isem.at[prompts + p])

    def out_copies(p):
        return [
            pltpu.make_async_copy(quad.at[p], quad_hbm.at[0, p], osem.at[prompts + p]),
            pltpu.make_async_copy(slow.at[p], slow_hbm.at[0, p], osem.at[2 * prompts + p]),
            pltpu.make_async_copy(nquad.at[p], nquad_hbm.at[0, p], osem.at[3 * prompts + p]),
            pltpu.make_async_copy(nlow.at[p], nlow_hbm.at[0, p], osem.at[4 * prompts + p]),
        ]

    def mixed_out(p):
        return pltpu.make_async_copy(mixed.at[p], mixed_hbm.at[p], osem.at[p])

    small = [
        pltpu.make_async_copy(low_hbm, low, isem.at[2 * prompts]),
        pltpu.make_async_copy(sel_hbm.at[pl.ds(pl.multiple_of(x * own, own), own)], sel, isem.at[2 * prompts + 1]),
    ]
    for p in range(prompts):
        mixed_in(p).start()
    small[0].start()
    small[1].start()
    for p in range(prompts):

        @pl.when(own_ref[p] == here)
        def _():
            fx_in(p).start()

        @pl.when(own_ref[p] != here)
        def _():
            quad[p] = jnp.zeros(quad.shape[1:], F32)
            slow[p] = jnp.zeros(slow.shape[1:], F32)
            nquad[p] = jnp.zeros(nquad.shape[1:], F32)
            nlow[p] = jnp.zeros(nlow.shape[1:], F32)
            for copy in out_copies(p):
                copy.start()

    for p in range(prompts):
        mixed_in(p).wait()
        mixed_out(p).start()

    small[0].wait()
    small[1].wait()
    quad_scale = (2.0 * FD) ** (-0.5)
    low_scale = FD ** (-0.25)
    lin, one = LIN - 128, ONE - 128
    for p in range(prompts):

        @pl.when(own_ref[p] == here)
        def _():
            fx_in(p).wait()
            first, rest = [], []
            for g in range(nx):
                for k in range(nc):
                    block = fx[k, p, g].astype(F32)
                    for i in range(2):
                        quad[p, g * HL + k * 2 + i] = block[i * own : (i + 1) * own] * quad_scale
                        at = 2 * own + i * 8 + NORM - (ROWS - 8)
                        first.append(block[at : at + 1])
                        rest.append(block[at + 1 : at + 2, : ROWS - 128])
            norms = jnp.concatenate([jnp.concatenate(first, axis=0), jnp.concatenate(rest, axis=0)], axis=1)
            nquad[p] = dot(norms.astype(BF16), sel[...], 1, 1) * quad_scale
            for k in range(nc):
                for i in range(2):
                    rows = low[k, p, i].astype(F32)
                    slow[p, 0, pl.ds(k * 2 + i, 1)] = rows[one : one + 1]
                    for r in range(FD):
                        slow[p, 1 + r, pl.ds(k * 2 + i, 1)] = rows[lin + r : lin + r + 1] * low_scale
                    tail = rows[NORM + 1 - 128 : NORM + 2 - 128]
                    nlow[p, pl.ds(k * 2 + i, 1)] = jnp.concatenate(
                        [tail[:, one : one + 1], tail[:, lin : lin + FD] * low_scale], axis=1
                    )
            for copy in out_copies(p):
                copy.start()

    for p in range(prompts):
        mixed_out(p).wait()
        for copy in out_copies(p):
            copy.wait()


def body(hidden_in, w_query, w_key, w_value, lengths, owners):
    nz, ny, nc, nx = (lax.axis_size(a) for a in ("z", "y", "c", "x"))
    prompts, span, width = hidden_in.shape
    own = FD // nx * FD
    part = 2 * own + 16
    zr = 2 * ROWS // nz
    wide = HD * HL * nx
    eq, sel = (jnp.asarray(t) for t in tables(nx))
    anyspace = pl.BlockSpec(memory_space=pl.ANY)
    scalars = pl.BlockSpec(memory_space=pltpu.SMEM)
    dma = pltpu.SemaphoreType.DMA

    def vmem(*shape, kind=BF16):
        return pltpu.VMEM(shape, kind)

    def array(*shape, kind=F32):
        return jax.ShapeDtypeStruct(shape, kind)

    block = (2, ROWS, HD)
    scaled, fx, low = pl.pallas_call(
        functools.partial(kernel, (nz, ny, nc, nx, span, wide)),
        out_shape=(
            array(prompts, span, HL * HD, kind=BF16),
            array(nc, prompts, nx, part, HD, kind=BF16),
            array(nc, prompts, 2, ROWS - 128, HD, kind=BF16),
        ),
        in_specs=[scalars] + [anyspace] * 6,
        out_specs=(anyspace,) * 3,
        scratch_shapes=[
            vmem(prompts, span, width), vmem(width, HL * HD), vmem(width, 128), vmem(128, width), vmem(width, 128),
            vmem(*eq.shape), vmem(*sel.shape),
            vmem(prompts, span, HL * HD), vmem(prompts, 128, span), vmem(span // 128, HL, 2 * FD, 128, kind=F32),
            vmem(prompts, HL, span, ROWS),
            vmem(prompts, HL, span, HD, kind=F32), vmem(prompts, HL, span, HD, kind=F32),
            vmem(prompts, HL, span, HD, kind=F32),
            vmem(prompts, span, HL * HD), vmem(8, span, kind=F32), vmem(nx, 8, span, kind=F32),
            vmem(prompts, 2, *block), vmem(prompts, *block), vmem(prompts, *block), vmem(ny, *block),
            vmem(nz, zr, HD), vmem(nz, zr, HD), vmem(nz, zr, HD), vmem(nz, zr, HD), vmem(zr, HD), vmem(nz, zr, HD),
            vmem(ny, *block), vmem(prompts, *block), vmem(prompts, *block), vmem(prompts, *block),
            vmem(nx, part, HD), vmem(prompts, nx, part, HD), vmem(prompts, 2, ROWS - 128, HD),
            dma((5,)), dma((prompts,)), dma((prompts,)), dma((prompts,)),
            dma((ny,)), dma((ny,)), dma((nz,)), dma((nz,)), dma((nz,)), dma((nz,)), dma((nz,)), dma((nz,)),
            dma((ny,)), dma((ny,)), dma((prompts,)), dma((prompts,)),
            dma((nx,)), dma((nx,)), dma((ny,)), dma((ny,)), dma((ny,)), dma((ny,)),
            dma((ny,)), dma((ny,)), dma((ny,)), dma((ny,)),
            dma((nx,)), dma((nx,)), dma((3 * prompts + 1,)),
        ],
        compiler_params=pltpu.CompilerParams(
            collective_id=0, has_side_effects=True, vmem_limit_bytes=60 * 1024 * 1024
        ),
        name="prefill",
    )(lengths, hidden_in, w_value, w_key, w_query, eq, sel)

    mixed, quad, state_low, nquad, nlow = pl.pallas_call(
        functools.partial(finish, (nz, ny, nc, nx, prompts)),
        out_shape=(
            array(prompts, span, HL * HD, kind=BF16),
            array(1, prompts, HL * nx, own, HD),
            array(1, prompts, FD + 1, HL, HD),
            array(1, prompts, HL * nx, own),
            array(1, prompts, HL, FD + 1),
        ),
        in_specs=[scalars] + [anyspace] * 4,
        out_specs=(anyspace,) * 5,
        scratch_shapes=[
            vmem(nc, prompts, nx, part, HD),
            vmem(nc, prompts, 2, ROWS - 128, HD), vmem(own, ROWS), vmem(prompts, span, HL * HD),
            vmem(prompts, HL * nx, own, HD, kind=F32), vmem(prompts, FD + 1, HL, HD, kind=F32),
            vmem(prompts, HL * nx, own, kind=F32), vmem(prompts, HL, FD + 1, kind=F32),
            dma((2 * prompts + 2,)), dma((5 * prompts,)),
        ],
        compiler_params=pltpu.CompilerParams(vmem_limit_bytes=60 * 1024 * 1024),
        name="finish",
    )(owners, scaled, fx, low, sel)
    return mixed, quad, jnp.transpose(state_low, (0, 1, 3, 2, 4)), nquad, nlow


def torus_of(mesh, shape=(8, 4, 2, 4)):
    return Mesh(mesh.devices.reshape(shape), ("z", "y", "c", "x"))


def run_on(torus):
    return jax.shard_map(
        body,
        mesh=torus,
        in_specs=(P(None, SEQ, None), P(), P(), P(None, "x"), P(), P()),
        out_specs=(
            P(None, SEQ, "x"),
            P(SEQ, None, None, "x", None),
            P(SEQ, None, "x", None, None),
            P(SEQ, None, None, "x"),
            P(SEQ, None, "x", None),
        ),
        check_vma=False,
    )


def solution(mesh):
    ny, nc = 4, 2
    feat = mesh.shape["feat"]
    return run_on(torus_of(mesh, (mesh.shape["seq"] // (ny * nc), ny, nc, feat)))
```

```python
import functools

import jax
import jax.numpy as jnp
import numpy as np
from jax import lax
from jax.experimental import pallas as pl
from jax.experimental.pallas import tpu as pltpu
from jax.sharding import Mesh
from jax.sharding import PartitionSpec as P

MESH = pl.DeviceIdType.MESH
F32, BF16 = jnp.float32, jnp.bfloat16
FD = 16
ROWS = 160
LIN, ONE, NORM = 136, 152, 153
HD = 128
NORM_FLOOR = 0.0001
HL = 4
SEQ = ("z", "y", "c")
LIMIT1, LIMIT2 = 44 << 20, 16 << 20


def packed_pairs():
    pairs = [(i, (i + d) % FD, d) for d in range(8) for i in range(FD)]
    return pairs + [(i, i + 8, 8) for i in range(8)]


def row_of(i, j):
    d = (j - i) % FD
    if d < 8:
        return d * FD + i
    if d == 8:
        return 8 * FD + min(i, j)
    return (FD - d) * FD + j


@functools.cache
def tables(nx):
    eq = np.zeros((2, HL, 128, ROWS), np.float32)
    for h in range(HL):
        for r, (i, j, d) in enumerate(packed_pairs()):
            eq[0, h, h * FD + i, r] = 1.0 / 32 if d == 0 else 1.0 / 16
            eq[1, h, h * FD + j, r] = 1.0
        for i in range(FD):
            eq[0, h, h * FD + i, LIN + i] = 0.25
            eq[1, h, 65, LIN + i] = 1.0
        eq[0, h, 65, ONE] = eq[1, h, 65, ONE] = 1.0
    own = FD // nx
    sel = np.zeros((nx, own * FD, ROWS), np.float32)
    for x in range(nx):
        for ii in range(own):
            for j in range(FD):
                sel[x, ii * FD + j, row_of(x * own + ii, j)] = 1.0
    return (
        eq.reshape(2 * HL, 128, ROWS).astype(BF16),
        sel.reshape(-1, ROWS).astype(BF16),
    )


def dot(a, b, ca=1, cb=0):
    return lax.dot_general(a, b, (((ca,), (cb,)), ((), ())), preferred_element_type=F32)


def kernel(
    sizes, len_ref, hid_hbm, wv_hbm, wk_hbm, wq_hbm, eq_hbm, sel_hbm, mixed, fx_all, low_all,
    hid, wv, wk, wkt, wq, eq, sel, val, keyt, kd, phi, nself, dself, att, sq, rsq,
    loc, r0, csum, ry, cut, whole_total, rz, pz, rpz, tt, rtt, py, rpy, pc, rpc, fxs, fxa, lowa,
    lsem, hsem, s0, v0, sy, vy, sz, vz, sz2, vz2, sz3, vz3, sy2, vy2, s02, v02,
    sx, vx, sy3, vy3, sy4, vy4, s3, v3, s4, v4, sx2, vx2, osem,
):
    nz, ny, nc, nx, span, width = sizes
    width_in = wk.shape[0]
    zr = 2 * ROWS // nz
    z, y, c, x = (lax.axis_index(a) for a in ("z", "y", "c", "x"))
    other = 1 - c
    pos0 = ((z * ny + y) * nc + c) * span

    col = pl.multiple_of((x * (HL * FD)) // 128 * 128, 128)
    shift = lax.rem(x * (HL * FD), 128)

    def turn(s):
        return lax.rem(y + jnp.where(s == 0, 2, jnp.where(s == 1, 1, jnp.where(s == 2, 3, 0))), ny)

    def hid_copies(p):
        rows = span // 4
        return [
            pltpu.make_async_copy(hid_hbm.at[p, pl.ds(i * rows, rows)], hid.at[p, pl.ds(i * rows, rows)], hsem.at[p, i])
            for i in range(4)
        ]

    def start_hid(p):
        for copy in hid_copies(p):
            copy.start()

    deep = width_in // 4
    wk_loads = [
        pltpu.make_async_copy(
            wk_hbm.at[pl.ds(i * deep, deep), pl.ds(col, 128)], wk.at[pl.ds(i * deep, deep)], lsem.at[i]
        )
        for i in range(4)
    ]
    wv_loads = [
        pltpu.make_async_copy(wv_hbm.at[pl.ds(i * deep, deep)], wv.at[pl.ds(i * deep, deep)], lsem.at[4 + i])
        for i in range(4)
    ]
    loads = [
        pltpu.make_async_copy(wq_hbm.at[:, pl.ds(col, 128)], wq, lsem.at[8]),
        pltpu.make_async_copy(eq_hbm, eq, lsem.at[9]),
        pltpu.make_async_copy(sel_hbm, sel, lsem.at[10]),
    ]
    for load in wk_loads:
        load.start()
    start_hid(turn(0))
    for load in wv_loads:
        load.start()
    for s in range(1, ny):
        start_hid(turn(s))
    for load in loads:
        load.start()

    barrier = pltpu.get_barrier_semaphore()
    peers = [(z, y, other, x)]
    peers += [(z, lax.rem(y + d, ny), c, x) for d in range(1, ny)]
    peers += [(lax.rem(z + d, nz), y, c, x) for d in range(1, nz)]
    peers += [(z, y, c, lax.rem(x + d, nx)) for d in range(1, nx)]
    for peer in peers:
        pl.semaphore_signal(barrier, inc=1, device_id=peer, device_id_type=MESH)

    def remote(src, dst, send, recv, dev):
        return pltpu.make_async_remote_copy(
            src_ref=src, dst_ref=dst, send_sem=send, recv_sem=recv, device_id=dev, device_id_type=MESH
        )

    core = (z, y, other, x)

    def at_y(q):
        return (z, q, c, x)

    def at_z(q):
        return (q, y, c, x)

    def at_x(q):
        return (z, y, c, q)

    for i in range(4):
        wk_loads[i].wait()
        wkt[:, i * deep : (i + 1) * deep] = jnp.transpose(wk[i * deep : (i + 1) * deep])
    keyt[...] = jnp.zeros(keyt.shape, BF16)
    far_z = sorted(range(1, nz), key=lambda d: -min(d, nz - d))
    far_y = [d for d in (1, 3, 2) if d < ny]
    ones = jnp.ones((8, span), BF16)
    sq[...] = jnp.zeros(sq.shape, F32)

    def to_core(p):
        return remote(loc.at[p, other], r0.at[p], s0.at[p], v0.at[p], core)

    def sum_to_y(p):
        return remote(csum.at[p], ry.at[y], sy.at[p], vy.at[y], at_y(p))

    def slice_to(q):
        return remote(cut.at[q], rz.at[z], sz.at[q], vz.at[z], at_z(q))

    def chip(p, own):
        to_core(p).wait_recv()
        both = loc[p, c].astype(F32) + r0[p].astype(F32)
        csum[p] = both.astype(BF16)
        if not own:
            sum_to_y(p).start()

    def keys(s):
        p = turn(s)
        for copy in hid_copies(p):
            copy.wait()
        kt = dot(wkt[pl.ds(pl.multiple_of(shift, 64), HL * FD)], hid[p], 1, 1).astype(BF16).astype(F32)
        kt = kt * (lax.broadcasted_iota(jnp.int32, (HL * FD, span), 1) + pos0 < len_ref[p]).astype(F32)
        keyt[p, : HL * FD] = kt.astype(BF16)
        for h in range(HL):
            for t in range(span // 128):
                piece = kt[h * FD : (h + 1) * FD, t * 128 : (t + 1) * 128]
                kd[t, h, :FD] = piece
                kd[t, h, FD:] = piece

    def values(s):
        p = turn(s)
        val[p] = dot(hid[p], wv[...]).astype(BF16)

    def state(s):
        p = turn(s)
        sub = lax.broadcasted_iota(jnp.int32, (8, 128), 0)
        for n in range(HL):
            pair = other if n < 2 else c
            h = pair * 2 + n % 2
            halves = []
            for t in range(span // 128):
                mine = kd[t, h, :FD]
                at = lax.broadcasted_iota(jnp.int32, (8, 128), 1) + (pos0 + t * 128)
                rows = [mine * kd[t, h, d : d + FD] for d in range(8)]
                rows += [mine[:8] * mine[8:], mine]
                rows += [jnp.where((sub == 0) & (at < len_ref[p]), 1.0, 0.0)]
                halves.append(jnp.concatenate(rows, axis=0).astype(BF16))
            feat = jnp.concatenate(halves, axis=1)
            st = dot(feat, val[p, :, pl.ds(pl.multiple_of(h * HD, HD), HD)])
            zn = dot(ones, feat, 1, 1)
            first = zn[:, :128]
            rest = jnp.concatenate([zn[:, 128:], jnp.zeros((8, 256 - ROWS), F32)], axis=1)
            tail = jnp.where(sub == 1, first, jnp.where(sub == 2, rest, st[ROWS - 8 :]))
            loc[p, pair, n % 2] = jnp.concatenate([st[: ROWS - 8], tail], axis=0).astype(BF16)
            if n == 1:
                to_core(p).start()

    keys(0)
    for load in wv_loads:
        load.wait()
    values(0)
    pl.semaphore_wait(barrier, len(peers))

    def step(s, carry):
        state(s)
        keys(s + 1)

        @pl.when(s == ny - 2)
        def _():
            chip(turn(s), False)

        values(s + 1)

        @pl.when(s < ny - 2)
        def _():
            chip(turn(s), False)

        return carry

    lax.fori_loop(0, ny - 1, step, 0)
    state(ny - 1)
    chip(y, True)
    ry[y] = csum[y]
    for d in range(1, ny):
        q = lax.rem(y + d, ny)
        remote(csum.at[q], ry.at[q], sy.at[q], vy.at[q], at_y(q)).wait_recv()
    total = ry[0].astype(F32)
    for q in range(1, ny):
        total = total + ry[q].astype(F32)
    whole_total[...] = total.reshape(2 * ROWS, HD)
    flat = whole_total[...]
    for q in range(nz):
        cut[q] = flat[q * zr : (q + 1) * zr].astype(BF16)
    for d in far_z:
        slice_to(lax.rem(z + d, nz)).start()
    rz[z] = cut[z]
    for load in loads:
        load.wait()

    def inside(p):
        q = pltpu.roll(dot(hid[p], wq[...]), shift, 1)
        lane = lax.broadcasted_iota(jnp.int32, (span, 128), 1)
        q = jnp.where(lane < HL * FD, q, jnp.where(lane == 65, 1.0, 0.0)).astype(BF16)
        t_at = lax.broadcasted_iota(jnp.int32, (span, span), 0)
        u_at = lax.broadcasted_iota(jnp.int32, (span, span), 1)
        seen = (u_at <= t_at) & (u_at + pos0 < len_ref[p])
        row = lax.broadcasted_iota(jnp.int32, (128, span), 0)
        kt = keyt[p]
        for h in range(HL):
            phi[p, h] = (dot(q, eq[h]) * dot(q, eq[HL + h])).astype(BF16)
            mine = jnp.where((row >= h * FD) & (row < (h + 1) * FD), kt, jnp.zeros_like(kt))
            half = dot(q, mine) * 0.25 + 1.0
            weight = jnp.where(seen, half * half * 0.5 + 0.5, 0.0).astype(BF16)
            nself[p, h] = dot(weight, val[p, :, h * HD : (h + 1) * HD])
            dself[p, h] = dot(weight, jnp.ones((span, HD), BF16))

    def inside_step(p, carry):
        inside(p)
        return carry

    lax.fori_loop(0, ny // 2, inside_step, 0)

    for d in range(1, nz):
        q = lax.rem(z + d, nz)
        remote(cut.at[q], rz.at[q], sz.at[q], vz.at[q], at_z(q)).wait_recv()
    run = jnp.zeros((zr, HD), F32)
    for q in range(nz):
        pz[q] = run.astype(BF16)
        run = run + rz[q].astype(F32)
    tt[...] = run.astype(BF16)

    def prefix_to_z(q):
        return remote(pz.at[q], rpz.at[z], sz2.at[q], vz2.at[z], at_z(q))

    def total_to_z(q):
        return remote(tt, rtt.at[z], sz3.at[q], vz3.at[z], at_z(q))

    for d in far_z:
        prefix_to_z(lax.rem(z + d, nz)).start()
    rpz[z] = pz[z]
    for d in far_z:
        total_to_z(lax.rem(z + d, nz)).start()
    rtt[z] = tt[...]

    lax.fori_loop(ny // 2, ny, inside_step, 0)

    for d in range(1, nz):
        q = lax.rem(z + d, nz)
        remote(pz.at[q], rpz.at[q], sz2.at[q], vz2.at[q], at_z(q)).wait_recv()
    run = jnp.concatenate([rpz[q].astype(F32) for q in range(nz)], axis=0).reshape(2, ROWS, HD)
    for q in range(ny):
        py[q] = run.astype(BF16)
        run = run + ry[q].astype(F32)

    def prefix_to_y(q):
        return remote(py.at[q], rpy.at[y], sy2.at[q], vy2.at[y], at_y(q))

    for d in far_y:
        prefix_to_y(lax.rem(y + d, ny)).start()
    rpy[y] = py[y]

    own = sel.shape[0] // nx
    for d in range(1, nz):
        q = lax.rem(z + d, nz)
        remote(tt, rtt.at[q], sz3.at[q], vz3.at[q], at_z(q)).wait_recv()
    whole = jnp.concatenate([rtt[q].astype(F32) for q in range(nz)], axis=0).reshape(2, ROWS, HD)
    tails = jnp.concatenate([whole[0, ROWS - 8 :], whole[1, ROWS - 8 :]], axis=0).astype(BF16)
    whole = whole.astype(BF16)
    for i in range(2):
        picked = dot(sel[...], whole[i]).astype(BF16)
        for q in range(nx):
            fxs[q, i * own : (i + 1) * own] = picked[q * own : (q + 1) * own]
        lowa[y, i] = whole[i, 128:]
    for q in range(nx):
        fxs[q, 2 * own :] = tails

    def final_to_x(q):
        return remote(fxs.at[q], fxa.at[y, x], sx.at[q], vx.at[x], at_x(q))

    for d in range(1, nx):
        final_to_x(lax.rem(x + d, nx)).start()
    fxa[y, x] = fxs[x]


    def attend(p, h, state):
        tail = state[ROWS - 8 :]
        norm = jnp.concatenate(
            [jnp.broadcast_to(tail[1:2], (HD, HD)), jnp.broadcast_to(tail[2:3, : ROWS - HD], (HD, ROWS - HD))], axis=1
        ).astype(BF16)
        feats = phi[p, h]
        num = dot(feats, state.astype(BF16)) + nself[p, h]
        den = dot(feats, norm, 1, 1) + dself[p, h]
        live = lax.broadcasted_iota(jnp.int32, (span, HD), 0) + pos0 < len_ref[p]
        att[p, h] = jnp.where(live, num / den, 0.0)

    def to_core2(p):
        return remote(pc.at[p], rpc.at[p], s02.at[p], v02.at[p], core)

    at_one = (c == 1).astype(F32)

    def near(p):
        chip = rpy[p].astype(F32)
        pc[p] = (chip + (1.0 - at_one) * loc[p, c].astype(F32)).astype(BF16)
        to_core2(p).start()
        mine = chip + at_one * r0[p].astype(F32)
        for i in range(2):
            attend(p, c * 2 + i, mine[i])

    def far(p):
        to_core2(p).wait_recv()
        there = rpc[p].astype(F32)
        for i in range(2):
            attend(p, other * 2 + i, there[i])
        square = att[p, 0] * att[p, 0]
        for h in range(1, HL):
            square = square + att[p, h] * att[p, h]
        high = square.astype(BF16)
        rest = (square - high.astype(F32)).astype(BF16)
        unit = jnp.ones((8, HD), BF16)
        sq[pl.ds(p, 1)] = (dot(unit, high, 1, 1) + dot(unit, rest, 1, 1))[0:1]

    def final_to_core(p):
        return remote(fxa.at[p], fx_all.at[c, p], s3.at[p], v3.at[p], core)

    def low_to_core(p):
        return remote(lowa.at[p], low_all.at[c, p], s4.at[p], v4.at[p], core)

    def final_here(p):
        return pltpu.make_async_copy(fxa.at[p], fx_all.at[c, p], osem.at[p])

    def low_here(p):
        return pltpu.make_async_copy(lowa.at[p], low_all.at[c, p], osem.at[ny + p])

    def deliver(p):
        for copy in (final_to_core(p), low_to_core(p), final_here(p), low_here(p)):
            copy.start()

    def arrived(d):
        p = lax.rem(y + d, ny)
        remote(py.at[p], rpy.at[p], sy2.at[p], vy2.at[p], at_y(p)).wait_recv()
        return p

    near(y)

    @pl.when(c == 0)
    def _():
        far(y)

    near(arrived(3))
    near(arrived(1))

    for d in range(1, nx):
        q = lax.rem(x + d, nx)
        remote(fxs.at[q], fxa.at[y, q], sx.at[q], vx.at[q], at_x(q)).wait_recv()

    def final_to_y(q):
        return remote(fxa.at[y], fxa.at[y], sy3.at[q], vy3.at[y], at_y(q))

    def low_to_y(q):
        return remote(lowa.at[y], lowa.at[y], sy4.at[q], vy4.at[y], at_y(q))

    for d in far_y:
        q = lax.rem(y + d, ny)
        final_to_y(q).start()
        low_to_y(q).start()

    deliver(y)

    @pl.when(c == 1)
    def _():
        far(y)

    far(lax.rem(y + 3, ny))
    near(arrived(2))
    far(lax.rem(y + 1, ny))
    far(lax.rem(y + 2, ny))

    def square_to_x(q):
        return remote(sq, rsq.at[x], sx2.at[q], vx2.at[x], at_x(q))

    for d in range(1, nx):
        square_to_x(lax.rem(x + d, nx)).start()

    rsq[x] = sq[...]
    for d in range(1, nx):
        q = lax.rem(x + d, nx)
        remote(sq, rsq.at[q], sx2.at[q], vx2.at[q], at_x(q)).wait_recv()

    squares = rsq[0]
    for q in range(1, nx):
        squares = squares + rsq[q]
    factor = jnp.transpose(lax.rsqrt(squares / width + NORM_FLOOR))
    for p in range(ny):
        scale = jnp.broadcast_to(factor[:, p : p + 1], (span, HD))
        for h in range(HL):
            mixed[p, :, h * HD : (h + 1) * HD] = (att[p, h] * scale).astype(BF16)

    for s in (3, 1, 2):
        q = lax.rem(y + s, ny)
        remote(fxa.at[y], fxa.at[q], sy3.at[q], vy3.at[q], at_y(q)).wait_recv()
        remote(lowa.at[y], lowa.at[q], sy4.at[q], vy4.at[q], at_y(q)).wait_recv()
        deliver(q)

    for p in range(ny):
        remote(fxa.at[p], fx_all.at[other, p], s3.at[p], v3.at[p], core).wait_recv()
        remote(lowa.at[p], low_all.at[other, p], s4.at[p], v4.at[p], core).wait_recv()

    for p in range(ny):
        to_core(p).wait_send()
        to_core2(p).wait_send()
    for d in range(1, ny):
        q = lax.rem(y + d, ny)
        sum_to_y(q).wait_send()
        prefix_to_y(q).wait_send()
        final_to_y(q).wait_send()
        low_to_y(q).wait_send()
    for d in range(1, nz):
        q = lax.rem(z + d, nz)
        slice_to(q).wait_send()
        prefix_to_z(q).wait_send()
        total_to_z(q).wait_send()
    for d in range(1, nx):
        q = lax.rem(x + d, nx)
        final_to_x(q).wait_send()
        square_to_x(q).wait_send()
    for p in range(ny):
        final_to_core(p).wait_send()
        low_to_core(p).wait_send()
        final_here(p).wait()
        low_here(p).wait()


def finish(
    sizes, own_ref, mixed, fx, low, sel_hbm, mixed_hbm, quad_hbm, slow_hbm, nquad_hbm, nlow_hbm,
    sel, quad, slow, nquad, nlow, isem, osem,
):
    nz, ny, nc, nx, prompts = sizes
    z, y, c, x = (lax.axis_index(a) for a in ("z", "y", "c", "x"))
    here = (z * ny + y) * nc + c
    own = sel.shape[0]

    def out_copies(p, at):
        return [
            pltpu.make_async_copy(quad.at[at], quad_hbm.at[0, p], osem.at[prompts + p]),
            pltpu.make_async_copy(slow.at[p], slow_hbm.at[0, p], osem.at[2 * prompts + p]),
            pltpu.make_async_copy(nquad.at[p], nquad_hbm.at[0, p], osem.at[3 * prompts + p]),
            pltpu.make_async_copy(nlow.at[p], nlow_hbm.at[0, p], osem.at[4 * prompts + p]),
        ]

    def mixed_out(p):
        return pltpu.make_async_copy(mixed.at[p], mixed_hbm.at[p], osem.at[p])

    sel_in = pltpu.make_async_copy(sel_hbm.at[pl.ds(pl.multiple_of(x * own, own), own)], sel, isem.at[0])
    sel_in.start()
    for p in range(prompts):
        mixed_out(p).start()
    quad[prompts] = jnp.zeros(quad.shape[1:], F32)
    slow[...] = jnp.zeros(slow.shape, F32)
    nquad[...] = jnp.zeros(nquad.shape, F32)
    nlow[...] = jnp.zeros(nlow.shape, F32)
    for p in range(prompts):

        @pl.when(own_ref[p] != here)
        def _():
            for copy in out_copies(p, prompts):
                copy.start()

    sel_in.wait()
    quad_scale = (2.0 * FD) ** (-0.5)
    low_scale = FD ** (-0.25)
    lin, one = LIN - 128, ONE - 128
    for p in range(prompts):

        @pl.when(own_ref[p] == here)
        def _():
            first, rest = [], []
            for g in range(nx):
                for k in range(nc):
                    block = fx[k, p, g].astype(F32)
                    for i in range(2):
                        quad[p, g * HL + k * 2 + i] = block[i * own : (i + 1) * own] * quad_scale
                        at = 2 * own + i * 8 + NORM - (ROWS - 8)
                        first.append(block[at : at + 1])
                        rest.append(block[at + 1 : at + 2, : ROWS - 128])
            norms = jnp.concatenate([jnp.concatenate(first, axis=0), jnp.concatenate(rest, axis=0)], axis=1)
            nquad[p] = dot(norms.astype(BF16), sel[...], 1, 1) * quad_scale
            for k in range(nc):
                for i in range(2):
                    rows = low[k, p, i].astype(F32)
                    slow[p, 0, pl.ds(k * 2 + i, 1)] = rows[one : one + 1]
                    for r in range(FD):
                        slow[p, 1 + r, pl.ds(k * 2 + i, 1)] = rows[lin + r : lin + r + 1] * low_scale
                    tail = rows[NORM + 1 - 128 : NORM + 2 - 128]
                    nlow[p, pl.ds(k * 2 + i, 1)] = jnp.concatenate(
                        [tail[:, one : one + 1], tail[:, lin : lin + FD] * low_scale], axis=1
                    )
            for copy in out_copies(p, p):
                copy.start()

    for p in range(prompts):
        mixed_out(p).wait()
        for copy in out_copies(p, p):
            copy.wait()


def body(hidden_in, w_query, w_key, w_value, lengths, owners):
    nz, ny, nc, nx = (lax.axis_size(a) for a in ("z", "y", "c", "x"))
    prompts, span, width = hidden_in.shape
    own = FD // nx * FD
    part = 2 * own + 16
    zr = 2 * ROWS // nz
    wide = HD * HL * nx
    eq, sel = (jnp.asarray(t) for t in tables(nx))
    lengths, owners, hidden_in, w_value, w_key, w_query, eq, sel = (
        pltpu.with_memory_space_constraint(a, pltpu.HBM)
        for a in (lengths, owners, hidden_in, w_value, w_key, w_query, eq, sel)
    )
    hbm = pl.BlockSpec(memory_space=pltpu.HBM)
    whole = pl.BlockSpec(memory_space=pltpu.VMEM)
    scalars = pl.BlockSpec(memory_space=pltpu.SMEM)
    dma = pltpu.SemaphoreType.DMA

    def vmem(*shape, kind=BF16):
        return pltpu.VMEM(shape, kind)

    def array(*shape, kind=F32):
        return jax.ShapeDtypeStruct(shape, kind)

    block = (2, ROWS, HD)
    scaled, fx, low = pl.pallas_call(
        functools.partial(kernel, (nz, ny, nc, nx, span, wide)),
        out_shape=(
            array(prompts, span, HL * HD, kind=BF16),
            array(nc, prompts, nx, part, HD, kind=BF16),
            array(nc, prompts, 2, ROWS - 128, HD, kind=BF16),
        ),
        in_specs=[scalars] + [hbm] * 6,
        out_specs=(whole,) * 3,
        scratch_shapes=[
            vmem(prompts, span, width), vmem(width, HL * HD), vmem(width, 128), vmem(128, width), vmem(width, 128),
            vmem(*eq.shape), vmem(*sel.shape),
            vmem(prompts, span, HL * HD), vmem(prompts, 128, span), vmem(span // 128, HL, 2 * FD, 128, kind=F32),
            vmem(prompts, HL, span, ROWS),
            vmem(prompts, HL, span, HD, kind=F32), vmem(prompts, HL, span, HD, kind=F32),
            vmem(prompts, HL, span, HD, kind=F32),
            vmem(8, span, kind=F32), vmem(nx, 8, span, kind=F32),
            vmem(prompts, 2, *block), vmem(prompts, *block), vmem(prompts, *block), vmem(ny, *block),
            vmem(nz, zr, HD), vmem(2 * ROWS, HD, kind=F32), vmem(nz, zr, HD),
            vmem(nz, zr, HD), vmem(nz, zr, HD), vmem(zr, HD), vmem(nz, zr, HD),
            vmem(ny, *block), vmem(prompts, *block), vmem(prompts, *block), vmem(prompts, *block),
            vmem(nx, part, HD), vmem(prompts, nx, part, HD), vmem(prompts, 2, ROWS - 128, HD),
            dma((11,)), dma((prompts, 4)), dma((prompts,)), dma((prompts,)),
            dma((ny,)), dma((ny,)), dma((nz,)), dma((nz,)), dma((nz,)), dma((nz,)), dma((nz,)), dma((nz,)),
            dma((ny,)), dma((ny,)), dma((prompts,)), dma((prompts,)),
            dma((nx,)), dma((nx,)), dma((ny,)), dma((ny,)), dma((ny,)), dma((ny,)),
            dma((ny,)), dma((ny,)), dma((ny,)), dma((ny,)),
            dma((nx,)), dma((nx,)), dma((2 * prompts,)),
        ],
        compiler_params=pltpu.CompilerParams(
            collective_id=0, has_side_effects=True, vmem_limit_bytes=LIMIT1
        ),
        name="prefill",
    )(lengths, hidden_in, w_value, w_key, w_query, eq, sel)

    mixed, quad, state_low, nquad, nlow = pl.pallas_call(
        functools.partial(finish, (nz, ny, nc, nx, prompts)),
        out_shape=(
            array(prompts, span, HL * HD, kind=BF16),
            array(1, prompts, HL * nx, own, HD),
            array(1, prompts, FD + 1, HL, HD),
            array(1, prompts, HL * nx, own),
            array(1, prompts, HL, FD + 1),
        ),
        in_specs=[scalars] + [whole] * 3 + [hbm],
        out_specs=(hbm,) * 5,
        scratch_shapes=[
            vmem(own, ROWS), vmem(prompts + 1, HL * nx, own, HD, kind=F32), vmem(prompts, FD + 1, HL, HD, kind=F32),
            vmem(prompts, HL * nx, own, kind=F32), vmem(prompts, HL, FD + 1, kind=F32),
            dma((1,)), dma((5 * prompts,)),
        ],
        compiler_params=pltpu.CompilerParams(vmem_limit_bytes=LIMIT2),
        name="finish",
    )(owners, scaled, fx, low, sel)
    return mixed, quad, jnp.transpose(state_low, (0, 1, 3, 2, 4)), nquad, nlow


def torus_of(mesh, shape=(8, 4, 2, 4)):
    return Mesh(mesh.devices.reshape(shape), ("z", "y", "c", "x"))


def run_on(torus):
    return jax.shard_map(
        body,
        mesh=torus,
        in_specs=(P(None, SEQ, None), P(), P(), P(None, "x"), P(), P()),
        out_specs=(
            P(None, SEQ, "x"),
            P(SEQ, None, None, "x", None),
            P(SEQ, None, "x", None, None),
            P(SEQ, None, None, "x"),
            P(SEQ, None, "x", None),
        ),
        check_vma=False,
    )


def solution(mesh):
    ny, nc = 4, 2
    feat = mesh.shape["feat"]
    return run_on(torus_of(mesh, (mesh.shape["seq"] // (ny * nc), ny, nc, feat)))
```

```python
import functools

import jax
import jax.numpy as jnp
import numpy as np
from jax import lax
from jax.experimental import pallas as pl
from jax.experimental.pallas import tpu as pltpu
from jax.sharding import Mesh
from jax.sharding import PartitionSpec as P

MESH = pl.DeviceIdType.MESH
F32, BF16 = jnp.float32, jnp.bfloat16
FD = 16
ROWS = 160
LIN, ONE, NORM = 136, 152, 153
HD = 128
NORM_FLOOR = 0.0001
HL = 4
SEQ = ("z", "y", "c")
LIMIT1, LIMIT2 = 44 << 20, 16 << 20


def packed_pairs():
    pairs = [(i, (i + d) % FD, d) for d in range(8) for i in range(FD)]
    return pairs + [(i, i + 8, 8) for i in range(8)]


def row_of(i, j):
    d = (j - i) % FD
    if d < 8:
        return d * FD + i
    if d == 8:
        return 8 * FD + min(i, j)
    return (FD - d) * FD + j


def needed(x, nx):
    own = FD // nx
    return sorted({row_of(x * own + n // FD, n % FD) for n in range(own * FD)})


def final_rows(nx):
    return -(-(2 * len(needed(0, nx)) + 4) // 16) * 16


@functools.cache
def tables(nx):
    eq = np.zeros((2, HL, 128, ROWS), np.float32)
    for h in range(HL):
        for r, (i, j, d) in enumerate(packed_pairs()):
            eq[0, h, h * FD + i, r] = 1.0 / 32 if d == 0 else 1.0 / 16
            eq[1, h, h * FD + j, r] = 1.0
        for i in range(FD):
            eq[0, h, h * FD + i, LIN + i] = 0.25
            eq[1, h, 65, LIN + i] = 1.0
        eq[0, h, 65, ONE] = eq[1, h, 65, ONE] = 1.0
    own = FD // nx
    part = final_rows(nx)
    sel = np.zeros((nx, part, 2 * ROWS), np.float32)
    spread = np.zeros((nx, 2 * own * FD, part), np.float32)
    pick = np.zeros((nx, own * FD, ROWS), np.float32)
    for x in range(nx):
        rows = needed(x, nx)
        for i in range(2):
            for n, r in enumerate(rows):
                sel[x, i * len(rows) + n, i * ROWS + r] = 1.0
            for r in range(2):
                sel[x, 2 * len(rows) + 2 * i + r, i * ROWS + NORM + r] = 1.0
            for n in range(own * FD):
                r = row_of(x * own + n // FD, n % FD)
                spread[x, i * own * FD + n, i * len(rows) + rows.index(r)] = 1.0
                pick[x, n, r] = 1.0
    return (
        eq.reshape(2 * HL, 128, ROWS).astype(BF16),
        sel.reshape(-1, 2 * ROWS).astype(BF16),
        spread.reshape(-1, part).astype(BF16),
        pick.reshape(-1, ROWS).astype(BF16),
    )


def dot(a, b, ca=1, cb=0):
    return lax.dot_general(a, b, (((ca,), (cb,)), ((), ())), preferred_element_type=F32)


def kernel(
    sizes, len_ref, hid_hbm, wv_hbm, wk_hbm, wq_hbm, eq_hbm, sel_hbm, mixed, fx_all, low_all,
    hid, wv, wk, wkt, wq, eq, sel, val, keyt, kd, phi, nself, dself, att, sq, rsq,
    loc, r0, csum, ry, cut, whole_total, rz, pz, rpz, tt, rtt, py, rpy, pc, rpc, fxs, fxa, lowa,
    lsem, hsem, s0, v0, sy, vy, sz, vz, sz2, vz2, sz3, vz3, sy2, vy2, s02, v02,
    sx, vx, sy3, vy3, sy4, vy4, s3, v3, s4, v4, sx2, vx2, osem,
):
    nz, ny, nc, nx, span, width = sizes
    width_in = wk.shape[0]
    zr = 2 * ROWS // nz
    z, y, c, x = (lax.axis_index(a) for a in ("z", "y", "c", "x"))
    other = 1 - c
    pos0 = ((z * ny + y) * nc + c) * span

    col = pl.multiple_of((x * (HL * FD)) // 128 * 128, 128)
    shift = lax.rem(x * (HL * FD), 128)

    def turn(s):
        return lax.rem(y + jnp.where(s == 0, 2, jnp.where(s == 1, 1, jnp.where(s == 2, 3, 0))), ny)

    def hid_copies(p):
        rows = span // 4
        return [
            pltpu.make_async_copy(hid_hbm.at[p, pl.ds(i * rows, rows)], hid.at[p, pl.ds(i * rows, rows)], hsem.at[p, i])
            for i in range(4)
        ]

    def start_hid(p):
        for copy in hid_copies(p):
            copy.start()

    deep = width_in // 4
    wk_loads = [
        pltpu.make_async_copy(
            wk_hbm.at[pl.ds(i * deep, deep), pl.ds(col, 128)], wk.at[pl.ds(i * deep, deep)], lsem.at[i]
        )
        for i in range(4)
    ]
    wv_loads = [
        pltpu.make_async_copy(wv_hbm.at[pl.ds(i * deep, deep)], wv.at[pl.ds(i * deep, deep)], lsem.at[4 + i])
        for i in range(4)
    ]
    loads = [
        pltpu.make_async_copy(wq_hbm.at[:, pl.ds(col, 128)], wq, lsem.at[8]),
        pltpu.make_async_copy(eq_hbm, eq, lsem.at[9]),
        pltpu.make_async_copy(sel_hbm, sel, lsem.at[10]),
    ]
    for load in wk_loads:
        load.start()
    start_hid(turn(0))
    for load in wv_loads:
        load.start()
    for s in range(1, ny):
        start_hid(turn(s))
    for load in loads:
        load.start()

    barrier = pltpu.get_barrier_semaphore()
    peers = [(z, y, other, x)]
    peers += [(z, lax.rem(y + d, ny), c, x) for d in range(1, ny)]
    peers += [(lax.rem(z + d, nz), y, c, x) for d in range(1, nz)]
    peers += [(z, y, c, lax.rem(x + d, nx)) for d in range(1, nx)]
    for peer in peers:
        pl.semaphore_signal(barrier, inc=1, device_id=peer, device_id_type=MESH)

    def remote(src, dst, send, recv, dev):
        return pltpu.make_async_remote_copy(
            src_ref=src, dst_ref=dst, send_sem=send, recv_sem=recv, device_id=dev, device_id_type=MESH
        )

    core = (z, y, other, x)

    def at_y(q):
        return (z, q, c, x)

    def at_z(q):
        return (q, y, c, x)

    def at_x(q):
        return (z, y, c, q)

    for i in range(4):
        wk_loads[i].wait()
        wkt[:, i * deep : (i + 1) * deep] = jnp.transpose(wk[i * deep : (i + 1) * deep])
    keyt[...] = jnp.zeros(keyt.shape, BF16)
    far_z = sorted(range(1, nz), key=lambda d: -min(d, nz - d))
    far_y = [d for d in (1, 3, 2) if d < ny]
    far_x = [d for d in (2, 1, 3) if d < nx]
    ones = jnp.ones((8, span), BF16)
    sq[...] = jnp.zeros(sq.shape, F32)

    def to_core(p):
        return remote(loc.at[p, other], r0.at[p], s0.at[p], v0.at[p], core)

    def sum_to_y(p):
        return remote(csum.at[p], ry.at[y], sy.at[p], vy.at[y], at_y(p))

    def slice_to(q):
        return remote(cut.at[q], rz.at[z], sz.at[q], vz.at[z], at_z(q))

    def chip(p, own):
        to_core(p).wait_recv()
        both = loc[p, c].astype(F32) + r0[p].astype(F32)
        csum[p] = both.astype(BF16)
        if not own:
            sum_to_y(p).start()

    def keys(s):
        p = turn(s)
        for copy in hid_copies(p):
            copy.wait()
        kt = dot(wkt[pl.ds(pl.multiple_of(shift, 64), HL * FD)], hid[p], 1, 1).astype(BF16).astype(F32)
        kt = kt * (lax.broadcasted_iota(jnp.int32, (HL * FD, span), 1) + pos0 < len_ref[p]).astype(F32)
        keyt[p, : HL * FD] = kt.astype(BF16)
        for h in range(HL):
            for t in range(span // 128):
                piece = kt[h * FD : (h + 1) * FD, t * 128 : (t + 1) * 128]
                kd[t, h, :FD] = piece
                kd[t, h, FD:] = piece

    def values(s):
        p = turn(s)
        val[p] = dot(hid[p], wv[...]).astype(BF16)

    def state(s):
        p = turn(s)
        sub = lax.broadcasted_iota(jnp.int32, (8, 128), 0)
        for n in range(HL):
            pair = other if n < 2 else c
            h = pair * 2 + n % 2
            halves = []
            for t in range(span // 128):
                mine = kd[t, h, :FD]
                at = lax.broadcasted_iota(jnp.int32, (8, 128), 1) + (pos0 + t * 128)
                rows = [mine * kd[t, h, d : d + FD] for d in range(8)]
                rows += [mine[:8] * mine[8:], mine]
                rows += [jnp.where((sub == 0) & (at < len_ref[p]), 1.0, 0.0)]
                halves.append(jnp.concatenate(rows, axis=0).astype(BF16))
            feat = jnp.concatenate(halves, axis=1)
            st = dot(feat, val[p, :, pl.ds(pl.multiple_of(h * HD, HD), HD)])
            zn = dot(ones, feat, 1, 1)
            first = zn[:, :128]
            rest = jnp.concatenate([zn[:, 128:], jnp.zeros((8, 256 - ROWS), F32)], axis=1)
            tail = jnp.where(sub == 1, first, jnp.where(sub == 2, rest, st[ROWS - 8 :]))
            loc[p, pair, n % 2] = jnp.concatenate([st[: ROWS - 8], tail], axis=0).astype(BF16)
            if n == 1:
                to_core(p).start()

    keys(0)
    for load in wv_loads:
        load.wait()
    values(0)
    pl.semaphore_wait(barrier, len(peers))

    def step(s, carry):
        state(s)
        keys(s + 1)

        @pl.when(s == ny - 2)
        def _():
            chip(turn(s), False)

        values(s + 1)

        @pl.when(s < ny - 2)
        def _():
            chip(turn(s), False)

        return carry

    lax.fori_loop(0, ny - 1, step, 0)
    state(ny - 1)
    chip(y, True)
    ry[y] = csum[y]
    for load in loads:
        load.wait()

    def inside(p):
        q = pltpu.roll(dot(hid[p], wq[...]), shift, 1)
        lane = lax.broadcasted_iota(jnp.int32, (span, 128), 1)
        q = jnp.where(lane < HL * FD, q, jnp.where(lane == 65, 1.0, 0.0)).astype(BF16)
        t_at = lax.broadcasted_iota(jnp.int32, (span, span), 0)
        u_at = lax.broadcasted_iota(jnp.int32, (span, span), 1)
        seen = (u_at <= t_at) & (u_at + pos0 < len_ref[p])
        row = lax.broadcasted_iota(jnp.int32, (128, span), 0)
        kt = keyt[p]
        for h in range(HL):
            phi[p, h] = (dot(q, eq[h]) * dot(q, eq[HL + h])).astype(BF16)
            mine = jnp.where((row >= h * FD) & (row < (h + 1) * FD), kt, jnp.zeros_like(kt))
            half = dot(q, mine) * 0.25 + 1.0
            weight = jnp.where(seen, half * half * 0.5 + 0.5, 0.0).astype(BF16)
            nself[p, h] = dot(weight, val[p, :, h * HD : (h + 1) * HD])
            dself[p, h] = dot(weight, jnp.ones((span, HD), BF16))

    def inside_step(p, carry):
        inside(p)
        return carry

    lax.fori_loop(0, 1, inside_step, 0)
    for d in range(1, ny):
        q = lax.rem(y + d, ny)
        remote(csum.at[q], ry.at[q], sy.at[q], vy.at[q], at_y(q)).wait_recv()
    total = ry[0].astype(F32)
    for q in range(1, ny):
        total = total + ry[q].astype(F32)
    whole_total[...] = total.reshape(2 * ROWS, HD)
    flat = whole_total[...]
    for q in range(nz):
        cut[q] = flat[q * zr : (q + 1) * zr].astype(BF16)
    for d in far_z:
        slice_to(lax.rem(z + d, nz)).start()
    rz[z] = cut[z]
    lax.fori_loop(1, ny // 2, inside_step, 0)

    for d in range(1, nz):
        q = lax.rem(z + d, nz)
        remote(cut.at[q], rz.at[q], sz.at[q], vz.at[q], at_z(q)).wait_recv()
    run = jnp.zeros((zr, HD), F32)
    for q in range(nz):
        pz[q] = run.astype(BF16)
        run = run + rz[q].astype(F32)
    tt[...] = run.astype(BF16)

    def prefix_to_z(q):
        return remote(pz.at[q], rpz.at[z], sz2.at[q], vz2.at[z], at_z(q))

    def total_to_z(q):
        return remote(tt, rtt.at[z], sz3.at[q], vz3.at[z], at_z(q))

    for d in far_z:
        prefix_to_z(lax.rem(z + d, nz)).start()
    rpz[z] = pz[z]
    for d in far_z:
        total_to_z(lax.rem(z + d, nz)).start()
    rtt[z] = tt[...]

    lax.fori_loop(ny // 2, ny, inside_step, 0)

    for d in range(1, nz):
        q = lax.rem(z + d, nz)
        remote(pz.at[q], rpz.at[q], sz2.at[q], vz2.at[q], at_z(q)).wait_recv()
    run = jnp.concatenate([rpz[q].astype(F32) for q in range(nz)], axis=0).reshape(2, ROWS, HD)
    for q in range(ny):
        py[q] = run.astype(BF16)
        run = run + ry[q].astype(F32)

    def prefix_to_y(q):
        return remote(py.at[q], rpy.at[y], sy2.at[q], vy2.at[y], at_y(q))

    for d in far_y:
        prefix_to_y(lax.rem(y + d, ny)).start()
    rpy[y] = py[y]

    part = sel.shape[0] // nx
    for d in range(1, nz):
        q = lax.rem(z + d, nz)
        remote(tt, rtt.at[q], sz3.at[q], vz3.at[q], at_z(q)).wait_recv()
    whole = jnp.concatenate([rtt[q] for q in range(nz)], axis=0) if zr % 16 == 0 else (
        jnp.concatenate([rtt[q].astype(F32) for q in range(nz)], axis=0).astype(BF16)
    )
    picked = dot(sel[...], whole).astype(BF16)
    for q in range(nx):
        fxs[q] = picked[q * part : (q + 1) * part]
    for i in range(2):
        lowa[y, i] = whole[i * ROWS + 128 : (i + 1) * ROWS]

    def final_to_x(q):
        return remote(fxs.at[q], fxa.at[y, x], sx.at[q], vx.at[x], at_x(q))

    for d in far_x:
        final_to_x(lax.rem(x + d, nx)).start()
    fxa[y, x] = fxs[x]


    def attend(p, h, state):
        tail = state[ROWS - 8 :]
        norm = jnp.concatenate(
            [jnp.broadcast_to(tail[1:2], (HD, HD)), jnp.broadcast_to(tail[2:3, : ROWS - HD], (HD, ROWS - HD))], axis=1
        ).astype(BF16)
        feats = phi[p, h]
        num = dot(feats, state.astype(BF16)) + nself[p, h]
        den = dot(feats, norm, 1, 1) + dself[p, h]
        live = lax.broadcasted_iota(jnp.int32, (span, HD), 0) + pos0 < len_ref[p]
        att[p, h] = jnp.where(live, num / den, 0.0)

    def to_core2(p):
        return remote(pc.at[p], rpc.at[p], s02.at[p], v02.at[p], core)

    at_one = (c == 1).astype(F32)

    def near(p):
        chip = rpy[p].astype(F32)
        pc[p] = (chip + (1.0 - at_one) * loc[p, c].astype(F32)).astype(BF16)
        to_core2(p).start()
        mine = chip + at_one * r0[p].astype(F32)
        for i in range(2):
            attend(p, c * 2 + i, mine[i])

    def far(p):
        to_core2(p).wait_recv()
        there = rpc[p].astype(F32)
        for i in range(2):
            attend(p, other * 2 + i, there[i])
        square = att[p, 0] * att[p, 0]
        for h in range(1, HL):
            square = square + att[p, h] * att[p, h]
        high = square.astype(BF16)
        rest = (square - high.astype(F32)).astype(BF16)
        unit = jnp.ones((8, HD), BF16)
        sq[pl.ds(p, 1)] = (dot(unit, high, 1, 1) + dot(unit, rest, 1, 1))[0:1]

    def final_to_core(p):
        return remote(fxa.at[p], fx_all.at[c, p], s3.at[p], v3.at[p], core)

    def low_to_core(p):
        return remote(lowa.at[p], low_all.at[c, p], s4.at[p], v4.at[p], core)

    def final_here(p):
        return pltpu.make_async_copy(fxa.at[p], fx_all.at[c, p], osem.at[p])

    def low_here(p):
        return pltpu.make_async_copy(lowa.at[p], low_all.at[c, p], osem.at[ny + p])

    def deliver(p):
        for copy in (final_to_core(p), low_to_core(p), final_here(p), low_here(p)):
            copy.start()

    def arrived(d):
        p = lax.rem(y + d, ny)
        remote(py.at[p], rpy.at[p], sy2.at[p], vy2.at[p], at_y(p)).wait_recv()
        return p

    near(y)

    @pl.when(c == 0)
    def _():
        far(y)

    near(arrived(3))
    near(arrived(1))

    for d in range(1, nx):
        q = lax.rem(x + d, nx)
        remote(fxs.at[q], fxa.at[y, q], sx.at[q], vx.at[q], at_x(q)).wait_recv()

    def final_to_y(q):
        return remote(fxa.at[y], fxa.at[y], sy3.at[q], vy3.at[y], at_y(q))

    def low_to_y(q):
        return remote(lowa.at[y], lowa.at[y], sy4.at[q], vy4.at[y], at_y(q))

    for d in far_y[::-1]:
        q = lax.rem(y + d, ny)
        final_to_y(q).start()
        low_to_y(q).start()

    deliver(y)

    @pl.when(c == 1)
    def _():
        far(y)

    far(lax.rem(y + 3, ny))
    near(arrived(2))
    far(lax.rem(y + 1, ny))
    far(lax.rem(y + 2, ny))

    def square_to_x(q):
        return remote(sq, rsq.at[x], sx2.at[q], vx2.at[x], at_x(q))

    for d in far_x:
        square_to_x(lax.rem(x + d, nx)).start()

    rsq[x] = sq[...]
    for d in range(1, nx):
        q = lax.rem(x + d, nx)
        remote(sq, rsq.at[q], sx2.at[q], vx2.at[q], at_x(q)).wait_recv()

    squares = rsq[0]
    for q in range(1, nx):
        squares = squares + rsq[q]
    factor = jnp.transpose(lax.rsqrt(squares / width + NORM_FLOOR))
    for p in range(ny):
        scale = jnp.broadcast_to(factor[:, p : p + 1], (span, HD))
        for h in range(HL):
            mixed[p, :, h * HD : (h + 1) * HD] = (att[p, h] * scale).astype(BF16)

    for s in (3, 1, 2):
        q = lax.rem(y + s, ny)
        remote(fxa.at[y], fxa.at[q], sy3.at[q], vy3.at[q], at_y(q)).wait_recv()
        remote(lowa.at[y], lowa.at[q], sy4.at[q], vy4.at[q], at_y(q)).wait_recv()
        deliver(q)

    for p in range(ny):
        remote(fxa.at[p], fx_all.at[other, p], s3.at[p], v3.at[p], core).wait_recv()
        remote(lowa.at[p], low_all.at[other, p], s4.at[p], v4.at[p], core).wait_recv()

    for p in range(ny):
        to_core(p).wait_send()
        to_core2(p).wait_send()
    for d in range(1, ny):
        q = lax.rem(y + d, ny)
        sum_to_y(q).wait_send()
        prefix_to_y(q).wait_send()
        final_to_y(q).wait_send()
        low_to_y(q).wait_send()
    for d in range(1, nz):
        q = lax.rem(z + d, nz)
        slice_to(q).wait_send()
        prefix_to_z(q).wait_send()
        total_to_z(q).wait_send()
    for d in range(1, nx):
        q = lax.rem(x + d, nx)
        final_to_x(q).wait_send()
        square_to_x(q).wait_send()
    for p in range(ny):
        final_to_core(p).wait_send()
        low_to_core(p).wait_send()
        final_here(p).wait()
        low_here(p).wait()


def finish(
    sizes, own_ref, mixed, fx, low, spread_hbm, pick_hbm, mixed_hbm, quad_hbm, slow_hbm, nquad_hbm, nlow_hbm,
    spread, pick, quad, slow, nquad, nlow, isem, osem,
):
    nz, ny, nc, nx, prompts = sizes
    z, y, c, x = (lax.axis_index(a) for a in ("z", "y", "c", "x"))
    here = (z * ny + y) * nc + c
    own = pick.shape[0]
    at_norm = 2 * len(needed(0, nx))

    def out_copies(p, at):
        return [
            pltpu.make_async_copy(quad.at[at], quad_hbm.at[0, p], osem.at[prompts + p]),
            pltpu.make_async_copy(slow.at[p], slow_hbm.at[0, p], osem.at[2 * prompts + p]),
            pltpu.make_async_copy(nquad.at[p], nquad_hbm.at[0, p], osem.at[3 * prompts + p]),
            pltpu.make_async_copy(nlow.at[p], nlow_hbm.at[0, p], osem.at[4 * prompts + p]),
        ]

    def mixed_out(p):
        return pltpu.make_async_copy(mixed.at[p], mixed_hbm.at[p], osem.at[p])

    tables_in = [
        pltpu.make_async_copy(
            spread_hbm.at[pl.ds(pl.multiple_of(x * 2 * own, 2 * own), 2 * own)], spread, isem.at[0]
        ),
        pltpu.make_async_copy(pick_hbm.at[pl.ds(pl.multiple_of(x * own, own), own)], pick, isem.at[1]),
    ]
    for table in tables_in:
        table.start()
    for p in range(prompts):
        mixed_out(p).start()
    quad[prompts] = jnp.zeros(quad.shape[1:], F32)
    slow[...] = jnp.zeros(slow.shape, F32)
    nquad[...] = jnp.zeros(nquad.shape, F32)
    nlow[...] = jnp.zeros(nlow.shape, F32)
    for p in range(prompts):

        @pl.when(own_ref[p] != here)
        def _():
            for copy in out_copies(p, prompts):
                copy.start()

    for table in tables_in:
        table.wait()
    quad_scale = (2.0 * FD) ** (-0.5)
    low_scale = FD ** (-0.25)
    lin, one = LIN - 128, ONE - 128
    for p in range(prompts):

        @pl.when(own_ref[p] == here)
        def _():
            first, rest = [], []
            for g in range(nx):
                for k in range(nc):
                    quads = dot(spread[...], fx[k, p, g])
                    norms = fx[k, p, g].astype(F32)
                    for i in range(2):
                        quad[p, g * HL + k * 2 + i] = quads[i * own : (i + 1) * own] * quad_scale
                        at = at_norm + 2 * i
                        first.append(norms[at : at + 1])
                        rest.append(norms[at + 1 : at + 2, : ROWS - 128])
            norms = jnp.concatenate([jnp.concatenate(first, axis=0), jnp.concatenate(rest, axis=0)], axis=1)
            nquad[p] = dot(norms.astype(BF16), pick[...], 1, 1) * quad_scale
            for k in range(nc):
                for i in range(2):
                    rows = low[k, p, i].astype(F32)
                    slow[p, 0, pl.ds(k * 2 + i, 1)] = rows[one : one + 1]
                    for r in range(FD):
                        slow[p, 1 + r, pl.ds(k * 2 + i, 1)] = rows[lin + r : lin + r + 1] * low_scale
                    tail = rows[NORM + 1 - 128 : NORM + 2 - 128]
                    nlow[p, pl.ds(k * 2 + i, 1)] = jnp.concatenate(
                        [tail[:, one : one + 1], tail[:, lin : lin + FD] * low_scale], axis=1
                    )
            for copy in out_copies(p, p):
                copy.start()

    for p in range(prompts):
        mixed_out(p).wait()
        for copy in out_copies(p, p):
            copy.wait()


def body(hidden_in, w_query, w_key, w_value, lengths, owners):
    nz, ny, nc, nx = (lax.axis_size(a) for a in ("z", "y", "c", "x"))
    prompts, span, width = hidden_in.shape
    own = FD // nx * FD
    part = final_rows(nx)
    zr = 2 * ROWS // nz
    wide = HD * HL * nx
    eq, sel, spread, pick = (jnp.asarray(t) for t in tables(nx))
    lengths, owners, hidden_in, w_value, w_key, w_query, eq, sel, spread, pick = (
        pltpu.with_memory_space_constraint(a, pltpu.HBM)
        for a in (lengths, owners, hidden_in, w_value, w_key, w_query, eq, sel, spread, pick)
    )
    hbm = pl.BlockSpec(memory_space=pltpu.HBM)
    whole = pl.BlockSpec(memory_space=pltpu.VMEM)
    scalars = pl.BlockSpec(memory_space=pltpu.SMEM)
    dma = pltpu.SemaphoreType.DMA

    def vmem(*shape, kind=BF16):
        return pltpu.VMEM(shape, kind)

    def array(*shape, kind=F32):
        return jax.ShapeDtypeStruct(shape, kind)

    block = (2, ROWS, HD)
    scaled, fx, low = pl.pallas_call(
        functools.partial(kernel, (nz, ny, nc, nx, span, wide)),
        out_shape=(
            array(prompts, span, HL * HD, kind=BF16),
            array(nc, prompts, nx, part, HD, kind=BF16),
            array(nc, prompts, 2, ROWS - 128, HD, kind=BF16),
        ),
        in_specs=[scalars] + [hbm] * 6,
        out_specs=(whole,) * 3,
        scratch_shapes=[
            vmem(prompts, span, width), vmem(width, HL * HD), vmem(width, 128), vmem(128, width), vmem(width, 128),
            vmem(*eq.shape), vmem(*sel.shape),
            vmem(prompts, span, HL * HD), vmem(prompts, 128, span), vmem(span // 128, HL, 2 * FD, 128, kind=F32),
            vmem(prompts, HL, span, ROWS),
            vmem(prompts, HL, span, HD, kind=F32), vmem(prompts, HL, span, HD, kind=F32),
            vmem(prompts, HL, span, HD, kind=F32),
            vmem(8, span, kind=F32), vmem(nx, 8, span, kind=F32),
            vmem(prompts, 2, *block), vmem(prompts, *block), vmem(prompts, *block), vmem(ny, *block),
            vmem(nz, zr, HD), vmem(2 * ROWS, HD, kind=F32), vmem(nz, zr, HD),
            vmem(nz, zr, HD), vmem(nz, zr, HD), vmem(zr, HD), vmem(nz, zr, HD),
            vmem(ny, *block), vmem(prompts, *block), vmem(prompts, *block), vmem(prompts, *block),
            vmem(nx, part, HD), vmem(prompts, nx, part, HD), vmem(prompts, 2, ROWS - 128, HD),
            dma((11,)), dma((prompts, 4)), dma((prompts,)), dma((prompts,)),
            dma((ny,)), dma((ny,)), dma((nz,)), dma((nz,)), dma((nz,)), dma((nz,)), dma((nz,)), dma((nz,)),
            dma((ny,)), dma((ny,)), dma((prompts,)), dma((prompts,)),
            dma((nx,)), dma((nx,)), dma((ny,)), dma((ny,)), dma((ny,)), dma((ny,)),
            dma((ny,)), dma((ny,)), dma((ny,)), dma((ny,)),
            dma((nx,)), dma((nx,)), dma((2 * prompts,)),
        ],
        compiler_params=pltpu.CompilerParams(
            collective_id=0, has_side_effects=True, vmem_limit_bytes=LIMIT1
        ),
        name="prefill",
    )(lengths, hidden_in, w_value, w_key, w_query, eq, sel)

    mixed, quad, state_low, nquad, nlow = pl.pallas_call(
        functools.partial(finish, (nz, ny, nc, nx, prompts)),
        out_shape=(
            array(prompts, span, HL * HD, kind=BF16),
            array(1, prompts, HL * nx, own, HD),
            array(1, prompts, FD + 1, HL, HD),
            array(1, prompts, HL * nx, own),
            array(1, prompts, HL, FD + 1),
        ),
        in_specs=[scalars] + [whole] * 3 + [hbm] * 2,
        out_specs=(hbm,) * 5,
        scratch_shapes=[
            vmem(2 * own, part), vmem(own, ROWS), vmem(prompts + 1, HL * nx, own, HD, kind=F32), vmem(prompts, FD + 1, HL, HD, kind=F32),
            vmem(prompts, HL * nx, own, kind=F32), vmem(prompts, HL, FD + 1, kind=F32),
            dma((2,)), dma((5 * prompts,)),
        ],
        compiler_params=pltpu.CompilerParams(vmem_limit_bytes=LIMIT2),
        name="finish",
    )(owners, scaled, fx, low, spread, pick)
    return mixed, quad, jnp.transpose(state_low, (0, 1, 3, 2, 4)), nquad, nlow


def torus_of(mesh, shape=(8, 4, 2, 4)):
    return Mesh(mesh.devices.reshape(shape), ("z", "y", "c", "x"))


def run_on(torus):
    return jax.shard_map(
        body,
        mesh=torus,
        in_specs=(P(None, SEQ, None), P(), P(), P(None, "x"), P(), P()),
        out_specs=(
            P(None, SEQ, "x"),
            P(SEQ, None, None, "x", None),
            P(SEQ, None, "x", None, None),
            P(SEQ, None, None, "x"),
            P(SEQ, None, "x", None),
        ),
        check_vma=False,
    )


def solution(mesh):
    ny, nc = 4, 2
    feat = mesh.shape["feat"]
    return run_on(torus_of(mesh, (mesh.shape["seq"] // (ny * nc), ny, nc, feat)))
```

```python
import functools

import jax
import jax.numpy as jnp
import numpy as np
from jax import lax
from jax.experimental import pallas as pl
from jax.experimental.pallas import tpu as pltpu
from jax.sharding import Mesh
from jax.sharding import PartitionSpec as P

MESH = pl.DeviceIdType.MESH
F32, BF16 = jnp.float32, jnp.bfloat16
FD = 16
ROWS = 160
LIN, ONE, NORM = 136, 152, 153
HD = 128
NORM_FLOOR = 0.0001
HL = 4
SEQ = ("z", "y", "c")
LIMIT1, LIMIT2 = 44 << 20, 16 << 20


def packed_pairs():
    pairs = [(i, (i + d) % FD, d) for d in range(8) for i in range(FD)]
    return pairs + [(i, i + 8, 8) for i in range(8)]


def row_of(i, j):
    d = (j - i) % FD
    if d < 8:
        return d * FD + i
    if d == 8:
        return 8 * FD + min(i, j)
    return (FD - d) * FD + j


def needed(x, nx):
    own = FD // nx
    return sorted({row_of(x * own + n // FD, n % FD) for n in range(own * FD)})


def final_rows(nx):
    return -(-(2 * len(needed(0, nx)) + 4) // 16) * 16


@functools.cache
def tables(nx):
    eq = np.zeros((2, HL, 128, ROWS), np.float32)
    for h in range(HL):
        for r, (i, j, d) in enumerate(packed_pairs()):
            eq[0, h, h * FD + i, r] = 1.0 / 32 if d == 0 else 1.0 / 16
            eq[1, h, h * FD + j, r] = 1.0
        for i in range(FD):
            eq[0, h, h * FD + i, LIN + i] = 0.25
            eq[1, h, 65, LIN + i] = 1.0
        eq[0, h, 65, ONE] = eq[1, h, 65, ONE] = 1.0
    own = FD // nx
    part = final_rows(nx)
    sel = np.zeros((nx, part, 2 * ROWS), np.float32)
    spread = np.zeros((nx, 2 * own * FD, part), np.float32)
    pick = np.zeros((nx, own * FD, ROWS), np.float32)
    for x in range(nx):
        rows = needed(x, nx)
        for i in range(2):
            for n, r in enumerate(rows):
                sel[x, i * len(rows) + n, i * ROWS + r] = 1.0
            for r in range(2):
                sel[x, 2 * len(rows) + 2 * i + r, i * ROWS + NORM + r] = 1.0
            for n in range(own * FD):
                r = row_of(x * own + n // FD, n % FD)
                spread[x, i * own * FD + n, i * len(rows) + rows.index(r)] = 1.0
                pick[x, n, r] = 1.0
    return (
        eq.reshape(2 * HL, 128, ROWS).astype(BF16),
        sel.reshape(-1, 2 * ROWS).astype(BF16),
        spread.reshape(-1, part).astype(BF16),
        pick.reshape(-1, ROWS).astype(BF16),
    )


def dot(a, b, ca=1, cb=0):
    return lax.dot_general(a, b, (((ca,), (cb,)), ((), ())), preferred_element_type=F32)


def kernel(
    sizes, len_ref, hid_hbm, wv_hbm, wk_hbm, wq_hbm, eq_hbm, sel_hbm, mixed, fx_all, low_all,
    hid, wv, wk, wkt, wq, eq, sel, val, keyt, kd, phi, nself, dself, att, sq, rsq,
    loc, r0, csum, ry, cut, whole_total, rz, pz, rpz, tt, rtt, py, rpy, pc, rpc, fxs,
    lsem, hsem, s0, v0, sy, vy, sz, vz, sz2, vz2, sz3, vz3, sy2, vy2, s02, v02,
    sx, vx, sy3, vy3, sy4, vy4, s3, v3, s4, v4, sx2, vx2,
):
    nz, ny, nc, nx, span, width = sizes
    width_in = wk.shape[0]
    zr = 2 * ROWS // nz
    z, y, c, x = (lax.axis_index(a) for a in ("z", "y", "c", "x"))
    other = 1 - c
    pos0 = ((z * ny + y) * nc + c) * span

    col = pl.multiple_of((x * (HL * FD)) // 128 * 128, 128)
    shift = lax.rem(x * (HL * FD), 128)

    def turn(s):
        return lax.rem(y + jnp.where(s == 0, 2, jnp.where(s == 1, 1, jnp.where(s == 2, 3, 0))), ny)

    def hid_copies(p):
        rows = span // 4
        return [
            pltpu.make_async_copy(hid_hbm.at[p, pl.ds(i * rows, rows)], hid.at[p, pl.ds(i * rows, rows)], hsem.at[p, i])
            for i in range(4)
        ]

    def start_hid(p):
        for copy in hid_copies(p):
            copy.start()

    deep = width_in // 4
    wk_loads = [
        pltpu.make_async_copy(
            wk_hbm.at[pl.ds(i * deep, deep), pl.ds(col, 128)], wk.at[pl.ds(i * deep, deep)], lsem.at[i]
        )
        for i in range(4)
    ]
    wv_loads = [
        pltpu.make_async_copy(wv_hbm.at[pl.ds(i * deep, deep)], wv.at[pl.ds(i * deep, deep)], lsem.at[4 + i])
        for i in range(4)
    ]
    loads = [
        pltpu.make_async_copy(wq_hbm.at[:, pl.ds(col, 128)], wq, lsem.at[8]),
        pltpu.make_async_copy(eq_hbm, eq, lsem.at[9]),
        pltpu.make_async_copy(sel_hbm, sel, lsem.at[10]),
    ]
    for load in wk_loads:
        load.start()
    start_hid(turn(0))
    for load in wv_loads:
        load.start()
    for s in range(1, ny):
        start_hid(turn(s))
    for load in loads:
        load.start()

    barrier = pltpu.get_barrier_semaphore()
    peers = [(z, y, other, x)]
    peers += [(z, lax.rem(y + d, ny), c, x) for d in range(1, ny)]
    peers += [(lax.rem(z + d, nz), y, c, x) for d in range(1, nz)]
    peers += [(z, y, c, lax.rem(x + d, nx)) for d in range(1, nx)]
    for peer in peers:
        pl.semaphore_signal(barrier, inc=1, device_id=peer, device_id_type=MESH)

    def remote(src, dst, send, recv, dev):
        return pltpu.make_async_remote_copy(
            src_ref=src, dst_ref=dst, send_sem=send, recv_sem=recv, device_id=dev, device_id_type=MESH
        )

    core = (z, y, other, x)

    def at_y(q):
        return (z, q, c, x)

    def at_z(q):
        return (q, y, c, x)

    def at_x(q):
        return (z, y, c, q)

    for i in range(4):
        wk_loads[i].wait()
        wkt[:, i * deep : (i + 1) * deep] = jnp.transpose(wk[i * deep : (i + 1) * deep])
    keyt[...] = jnp.zeros(keyt.shape, BF16)
    far_z = sorted(range(1, nz), key=lambda d: -min(d, nz - d))
    far_y = [d for d in (1, 3, 2) if d < ny]
    far_x = [d for d in (2, 1, 3) if d < nx]
    ones = jnp.ones((8, span), BF16)
    sq[...] = jnp.zeros(sq.shape, F32)

    def to_core(p):
        return remote(loc.at[p, other], r0.at[p], s0.at[p], v0.at[p], core)

    def sum_to_y(p):
        return remote(csum.at[p], ry.at[y], sy.at[p], vy.at[y], at_y(p))

    def slice_to(q):
        return remote(cut.at[q], rz.at[z], sz.at[q], vz.at[z], at_z(q))

    def chip(p, own):
        to_core(p).wait_recv()
        both = loc[p, c].astype(F32) + r0[p].astype(F32)
        csum[p] = both.astype(BF16)
        if not own:
            sum_to_y(p).start()

    def keys(s):
        p = turn(s)
        for copy in hid_copies(p):
            copy.wait()
        kt = dot(wkt[pl.ds(pl.multiple_of(shift, 64), HL * FD)], hid[p], 1, 1).astype(BF16).astype(F32)
        kt = kt * (lax.broadcasted_iota(jnp.int32, (HL * FD, span), 1) + pos0 < len_ref[p]).astype(F32)
        keyt[p, : HL * FD] = kt.astype(BF16)
        for h in range(HL):
            for t in range(span // 128):
                piece = kt[h * FD : (h + 1) * FD, t * 128 : (t + 1) * 128]
                kd[t, h, :FD] = piece
                kd[t, h, FD:] = piece

    def values(s):
        p = turn(s)
        val[p] = dot(hid[p], wv[...]).astype(BF16)

    def state(s):
        p = turn(s)
        sub = lax.broadcasted_iota(jnp.int32, (8, 128), 0)
        for n in range(HL):
            pair = other if n < 2 else c
            h = pair * 2 + n % 2
            halves = []
            for t in range(span // 128):
                mine = kd[t, h, :FD]
                at = lax.broadcasted_iota(jnp.int32, (8, 128), 1) + (pos0 + t * 128)
                rows = [mine * kd[t, h, d : d + FD] for d in range(8)]
                rows += [mine[:8] * mine[8:], mine]
                rows += [jnp.where((sub == 0) & (at < len_ref[p]), 1.0, 0.0)]
                halves.append(jnp.concatenate(rows, axis=0).astype(BF16))
            feat = jnp.concatenate(halves, axis=1)
            st = dot(feat, val[p, :, pl.ds(pl.multiple_of(h * HD, HD), HD)])
            zn = dot(ones, feat, 1, 1)
            first = zn[:, :128]
            rest = jnp.concatenate([zn[:, 128:], jnp.zeros((8, 256 - ROWS), F32)], axis=1)
            tail = jnp.where(sub == 1, first, jnp.where(sub == 2, rest, st[ROWS - 8 :]))
            loc[p, pair, n % 2] = jnp.concatenate([st[: ROWS - 8], tail], axis=0).astype(BF16)
            if n == 1:
                to_core(p).start()

    keys(0)
    for load in wv_loads:
        load.wait()
    values(0)
    pl.semaphore_wait(barrier, len(peers))

    def step(s, carry):
        state(s)
        keys(s + 1)

        @pl.when(s == ny - 2)
        def _():
            chip(turn(s), False)

        values(s + 1)

        @pl.when(s < ny - 2)
        def _():
            chip(turn(s), False)

        return carry

    lax.fori_loop(0, ny - 1, step, 0)
    state(ny - 1)
    chip(y, True)
    ry[y] = csum[y]
    for load in loads:
        load.wait()

    def inside(p):
        q = pltpu.roll(dot(hid[p], wq[...]), shift, 1)
        lane = lax.broadcasted_iota(jnp.int32, (span, 128), 1)
        q = jnp.where(lane < HL * FD, q, jnp.where(lane == 65, 1.0, 0.0)).astype(BF16)
        t_at = lax.broadcasted_iota(jnp.int32, (span, span), 0)
        u_at = lax.broadcasted_iota(jnp.int32, (span, span), 1)
        seen = (u_at <= t_at) & (u_at + pos0 < len_ref[p])
        row = lax.broadcasted_iota(jnp.int32, (128, span), 0)
        kt = keyt[p]
        for h in range(HL):
            phi[p, h] = (dot(q, eq[h]) * dot(q, eq[HL + h])).astype(BF16)
            mine = jnp.where((row >= h * FD) & (row < (h + 1) * FD), kt, jnp.zeros_like(kt))
            half = dot(q, mine) * 0.25 + 1.0
            weight = jnp.where(seen, half * half * 0.5 + 0.5, 0.0).astype(BF16)
            nself[p, h] = dot(weight, val[p, :, h * HD : (h + 1) * HD])
            dself[p, h] = dot(weight, jnp.ones((span, HD), BF16))

    def inside_step(p, carry):
        inside(p)
        return carry

    lax.fori_loop(0, 1, inside_step, 0)
    for d in range(1, ny):
        q = lax.rem(y + d, ny)
        remote(csum.at[q], ry.at[q], sy.at[q], vy.at[q], at_y(q)).wait_recv()
    total = ry[0].astype(F32)
    for q in range(1, ny):
        total = total + ry[q].astype(F32)
    whole_total[...] = total.reshape(2 * ROWS, HD)
    flat = whole_total[...]
    for q in range(nz):
        cut[q] = flat[q * zr : (q + 1) * zr].astype(BF16)
    for d in far_z:
        slice_to(lax.rem(z + d, nz)).start()
    rz[z] = cut[z]
    lax.fori_loop(1, ny // 2, inside_step, 0)

    for d in range(1, nz):
        q = lax.rem(z + d, nz)
        remote(cut.at[q], rz.at[q], sz.at[q], vz.at[q], at_z(q)).wait_recv()
    run = jnp.zeros((zr, HD), F32)
    for q in range(nz):
        pz[q] = run.astype(BF16)
        run = run + rz[q].astype(F32)
    tt[...] = run.astype(BF16)

    def prefix_to_z(q):
        return remote(pz.at[q], rpz.at[z], sz2.at[q], vz2.at[z], at_z(q))

    def total_to_z(q):
        return remote(tt, rtt.at[z], sz3.at[q], vz3.at[z], at_z(q))

    for d in far_z:
        prefix_to_z(lax.rem(z + d, nz)).start()
    rpz[z] = pz[z]
    for d in far_z:
        total_to_z(lax.rem(z + d, nz)).start()
    rtt[z] = tt[...]

    lax.fori_loop(ny // 2, ny, inside_step, 0)

    for d in range(1, nz):
        q = lax.rem(z + d, nz)
        remote(pz.at[q], rpz.at[q], sz2.at[q], vz2.at[q], at_z(q)).wait_recv()
    run = jnp.concatenate([rpz[q].astype(F32) for q in range(nz)], axis=0).reshape(2, ROWS, HD)
    for q in range(ny):
        py[q] = run.astype(BF16)
        run = run + ry[q].astype(F32)

    def prefix_to_y(q):
        return remote(py.at[q], rpy.at[y], sy2.at[q], vy2.at[y], at_y(q))

    for d in far_y:
        prefix_to_y(lax.rem(y + d, ny)).start()
    rpy[y] = py[y]

    part = sel.shape[0] // nx
    for d in range(1, nz):
        q = lax.rem(z + d, nz)
        remote(tt, rtt.at[q], sz3.at[q], vz3.at[q], at_z(q)).wait_recv()
    whole = jnp.concatenate([rtt[q] for q in range(nz)], axis=0) if zr % 16 == 0 else (
        jnp.concatenate([rtt[q].astype(F32) for q in range(nz)], axis=0).astype(BF16)
    )
    picked = dot(sel[...], whole).astype(BF16)
    for q in range(nx):
        fxs[q] = picked[q * part : (q + 1) * part]
    for i in range(2):
        low_all[c, y, i] = whole[i * ROWS + 128 : (i + 1) * ROWS]

    def final_to_x(q):
        return remote(fxs.at[q], fx_all.at[c, y, x], sx.at[q], vx.at[x], at_x(q))

    for d in far_x:
        final_to_x(lax.rem(x + d, nx)).start()
    fx_all[c, y, x] = fxs[x]


    def attend(p, h, state):
        tail = state[ROWS - 8 :]
        norm = jnp.concatenate(
            [jnp.broadcast_to(tail[1:2], (HD, HD)), jnp.broadcast_to(tail[2:3, : ROWS - HD], (HD, ROWS - HD))], axis=1
        ).astype(BF16)
        feats = phi[p, h]
        num = dot(feats, state.astype(BF16)) + nself[p, h]
        den = dot(feats, norm, 1, 1) + dself[p, h]
        live = lax.broadcasted_iota(jnp.int32, (span, HD), 0) + pos0 < len_ref[p]
        att[p, h] = jnp.where(live, num / den, 0.0)

    def to_core2(p):
        return remote(pc.at[p], rpc.at[p], s02.at[p], v02.at[p], core)

    at_one = (c == 1).astype(F32)

    def near(p):
        chip = rpy[p].astype(F32)
        pc[p] = (chip + (1.0 - at_one) * loc[p, c].astype(F32)).astype(BF16)
        to_core2(p).start()
        mine = chip + at_one * r0[p].astype(F32)
        for i in range(2):
            attend(p, c * 2 + i, mine[i])

    def far(p):
        to_core2(p).wait_recv()
        there = rpc[p].astype(F32)
        for i in range(2):
            attend(p, other * 2 + i, there[i])
        square = att[p, 0] * att[p, 0]
        for h in range(1, HL):
            square = square + att[p, h] * att[p, h]
        high = square.astype(BF16)
        rest = (square - high.astype(F32)).astype(BF16)
        unit = jnp.ones((8, HD), BF16)
        sq[pl.ds(p, 1)] = (dot(unit, high, 1, 1) + dot(unit, rest, 1, 1))[0:1]

    def final_to_core(p):
        return remote(fx_all.at[c, p], fx_all.at[c, p], s3.at[p], v3.at[p], core)

    def low_to_core(p):
        return remote(low_all.at[c, p], low_all.at[c, p], s4.at[p], v4.at[p], core)

    def deliver(p):
        final_to_core(p).start()
        low_to_core(p).start()

    def arrived(d):
        p = lax.rem(y + d, ny)
        remote(py.at[p], rpy.at[p], sy2.at[p], vy2.at[p], at_y(p)).wait_recv()
        return p

    near(y)

    @pl.when(c == 0)
    def _():
        far(y)

    near(arrived(3))
    near(arrived(1))

    for d in range(1, nx):
        q = lax.rem(x + d, nx)
        remote(fxs.at[q], fx_all.at[c, y, q], sx.at[q], vx.at[q], at_x(q)).wait_recv()

    def final_to_y(q):
        return remote(fx_all.at[c, y], fx_all.at[c, y], sy3.at[q], vy3.at[y], at_y(q))

    def low_to_y(q):
        return remote(low_all.at[c, y], low_all.at[c, y], sy4.at[q], vy4.at[y], at_y(q))

    for d in far_y[::-1]:
        q = lax.rem(y + d, ny)
        final_to_y(q).start()
    for d in far_y[::-1]:
        low_to_y(lax.rem(y + d, ny)).start()

    deliver(y)

    @pl.when(c == 1)
    def _():
        far(y)

    far(lax.rem(y + 3, ny))
    near(arrived(2))
    far(lax.rem(y + 1, ny))
    far(lax.rem(y + 2, ny))

    def square_to_x(q):
        return remote(sq, rsq.at[x], sx2.at[q], vx2.at[x], at_x(q))

    for d in far_x:
        square_to_x(lax.rem(x + d, nx)).start()

    rsq[x] = sq[...]
    for d in range(1, nx):
        q = lax.rem(x + d, nx)
        remote(sq, rsq.at[q], sx2.at[q], vx2.at[q], at_x(q)).wait_recv()

    squares = rsq[0]
    for q in range(1, nx):
        squares = squares + rsq[q]
    factor = jnp.transpose(lax.rsqrt(squares / width + NORM_FLOOR))
    for p in range(ny):
        scale = jnp.broadcast_to(factor[:, p : p + 1], (span, HD))
        for h in range(HL):
            mixed[p, :, h * HD : (h + 1) * HD] = (att[p, h] * scale).astype(BF16)

    for s in (3, 1, 2):
        q = lax.rem(y + s, ny)
        remote(fx_all.at[c, y], fx_all.at[c, q], sy3.at[q], vy3.at[q], at_y(q)).wait_recv()
        final_to_core(q).start()
    for s in (3, 1, 2):
        q = lax.rem(y + s, ny)
        remote(low_all.at[c, y], low_all.at[c, q], sy4.at[q], vy4.at[q], at_y(q)).wait_recv()
        low_to_core(q).start()

    for p in range(ny):
        remote(fx_all.at[c, p], fx_all.at[other, p], s3.at[p], v3.at[p], core).wait_recv()
        remote(low_all.at[c, p], low_all.at[other, p], s4.at[p], v4.at[p], core).wait_recv()

    for p in range(ny):
        to_core(p).wait_send()
        to_core2(p).wait_send()
    for d in range(1, ny):
        q = lax.rem(y + d, ny)
        sum_to_y(q).wait_send()
        prefix_to_y(q).wait_send()
        final_to_y(q).wait_send()
        low_to_y(q).wait_send()
    for d in range(1, nz):
        q = lax.rem(z + d, nz)
        slice_to(q).wait_send()
        prefix_to_z(q).wait_send()
        total_to_z(q).wait_send()
    for d in range(1, nx):
        q = lax.rem(x + d, nx)
        final_to_x(q).wait_send()
        square_to_x(q).wait_send()
    for p in range(ny):
        final_to_core(p).wait_send()
        low_to_core(p).wait_send()


def finish(
    sizes, own_ref, mixed, fx, low, spread_hbm, pick_hbm, mixed_hbm, quad_hbm, slow_hbm, nquad_hbm, nlow_hbm,
    spread, pick, quad, slow, nquad, nlow, isem, osem,
):
    nz, ny, nc, nx, prompts = sizes
    z, y, c, x = (lax.axis_index(a) for a in ("z", "y", "c", "x"))
    here = (z * ny + y) * nc + c
    own = pick.shape[0]
    at_norm = 2 * len(needed(0, nx))

    def out_copies(p, at):
        return [
            pltpu.make_async_copy(quad.at[at], quad_hbm.at[0, p], osem.at[prompts + p]),
            pltpu.make_async_copy(slow.at[p], slow_hbm.at[0, p], osem.at[2 * prompts + p]),
            pltpu.make_async_copy(nquad.at[p], nquad_hbm.at[0, p], osem.at[3 * prompts + p]),
            pltpu.make_async_copy(nlow.at[p], nlow_hbm.at[0, p], osem.at[4 * prompts + p]),
        ]

    def mixed_out(p):
        return pltpu.make_async_copy(mixed.at[p], mixed_hbm.at[p], osem.at[p])

    tables_in = [
        pltpu.make_async_copy(
            spread_hbm.at[pl.ds(pl.multiple_of(x * 2 * own, 2 * own), 2 * own)], spread, isem.at[0]
        ),
        pltpu.make_async_copy(pick_hbm.at[pl.ds(pl.multiple_of(x * own, own), own)], pick, isem.at[1]),
    ]
    for table in tables_in:
        table.start()
    for p in range(prompts):
        mixed_out(p).start()
    quad[prompts] = jnp.zeros(quad.shape[1:], F32)
    slow[...] = jnp.zeros(slow.shape, F32)
    nquad[...] = jnp.zeros(nquad.shape, F32)
    nlow[...] = jnp.zeros(nlow.shape, F32)
    for p in range(prompts):

        @pl.when(own_ref[p] != here)
        def _():
            for copy in out_copies(p, prompts):
                copy.start()

    for table in tables_in:
        table.wait()
    quad_scale = (2.0 * FD) ** (-0.5)
    low_scale = FD ** (-0.25)
    lin, one = LIN - 128, ONE - 128
    for p in range(prompts):

        @pl.when(own_ref[p] == here)
        def _():
            first, rest = [], []
            for g in range(nx):
                for k in range(nc):
                    quads = dot(spread[...], fx[k, p, g])
                    norms = fx[k, p, g].astype(F32)
                    for i in range(2):
                        quad[p, g * HL + k * 2 + i] = quads[i * own : (i + 1) * own] * quad_scale
                        at = at_norm + 2 * i
                        first.append(norms[at : at + 1])
                        rest.append(norms[at + 1 : at + 2, : ROWS - 128])
            norms = jnp.concatenate([jnp.concatenate(first, axis=0), jnp.concatenate(rest, axis=0)], axis=1)
            nquad[p] = dot(norms.astype(BF16), pick[...], 1, 1) * quad_scale
            for k in range(nc):
                for i in range(2):
                    rows = low[k, p, i].astype(F32)
                    slow[p, 0, pl.ds(k * 2 + i, 1)] = rows[one : one + 1]
                    for r in range(FD):
                        slow[p, 1 + r, pl.ds(k * 2 + i, 1)] = rows[lin + r : lin + r + 1] * low_scale
                    tail = rows[NORM + 1 - 128 : NORM + 2 - 128]
                    nlow[p, pl.ds(k * 2 + i, 1)] = jnp.concatenate(
                        [tail[:, one : one + 1], tail[:, lin : lin + FD] * low_scale], axis=1
                    )
            for copy in out_copies(p, p):
                copy.start()

    for p in range(prompts):
        mixed_out(p).wait()
        for copy in out_copies(p, p):
            copy.wait()


def body(hidden_in, w_query, w_key, w_value, lengths, owners):
    nz, ny, nc, nx = (lax.axis_size(a) for a in ("z", "y", "c", "x"))
    prompts, span, width = hidden_in.shape
    own = FD // nx * FD
    part = final_rows(nx)
    zr = 2 * ROWS // nz
    wide = HD * HL * nx
    eq, sel, spread, pick = (jnp.asarray(t) for t in tables(nx))
    lengths, owners, hidden_in, w_value, w_key, w_query, eq, sel, spread, pick = (
        pltpu.with_memory_space_constraint(a, pltpu.HBM)
        for a in (lengths, owners, hidden_in, w_value, w_key, w_query, eq, sel, spread, pick)
    )
    hbm = pl.BlockSpec(memory_space=pltpu.HBM)
    whole = pl.BlockSpec(memory_space=pltpu.VMEM)
    scalars = pl.BlockSpec(memory_space=pltpu.SMEM)
    dma = pltpu.SemaphoreType.DMA

    def vmem(*shape, kind=BF16):
        return pltpu.VMEM(shape, kind)

    def array(*shape, kind=F32):
        return jax.ShapeDtypeStruct(shape, kind)

    block = (2, ROWS, HD)
    scaled, fx, low = pl.pallas_call(
        functools.partial(kernel, (nz, ny, nc, nx, span, wide)),
        out_shape=(
            array(prompts, span, HL * HD, kind=BF16),
            array(nc, prompts, nx, part, HD, kind=BF16),
            array(nc, prompts, 2, ROWS - 128, HD, kind=BF16),
        ),
        in_specs=[scalars] + [hbm] * 6,
        out_specs=(whole,) * 3,
        scratch_shapes=[
            vmem(prompts, span, width), vmem(width, HL * HD), vmem(width, 128), vmem(128, width), vmem(width, 128),
            vmem(*eq.shape), vmem(*sel.shape),
            vmem(prompts, span, HL * HD), vmem(prompts, 128, span), vmem(span // 128, HL, 2 * FD, 128, kind=F32),
            vmem(prompts, HL, span, ROWS),
            vmem(prompts, HL, span, HD, kind=F32), vmem(prompts, HL, span, HD, kind=F32),
            vmem(prompts, HL, span, HD, kind=F32),
            vmem(8, span, kind=F32), vmem(nx, 8, span, kind=F32),
            vmem(prompts, 2, *block), vmem(prompts, *block), vmem(prompts, *block), vmem(ny, *block),
            vmem(nz, zr, HD), vmem(2 * ROWS, HD, kind=F32), vmem(nz, zr, HD),
            vmem(nz, zr, HD), vmem(nz, zr, HD), vmem(zr, HD), vmem(nz, zr, HD),
            vmem(ny, *block), vmem(prompts, *block), vmem(prompts, *block), vmem(prompts, *block),
            vmem(nx, part, HD),
            dma((11,)), dma((prompts, 4)), dma((prompts,)), dma((prompts,)),
            dma((ny,)), dma((ny,)), dma((nz,)), dma((nz,)), dma((nz,)), dma((nz,)), dma((nz,)), dma((nz,)),
            dma((ny,)), dma((ny,)), dma((prompts,)), dma((prompts,)),
            dma((nx,)), dma((nx,)), dma((ny,)), dma((ny,)), dma((ny,)), dma((ny,)),
            dma((ny,)), dma((ny,)), dma((ny,)), dma((ny,)),
            dma((nx,)), dma((nx,)),
        ],
        compiler_params=pltpu.CompilerParams(
            collective_id=0, has_side_effects=True, vmem_limit_bytes=LIMIT1
        ),
        name="prefill",
    )(lengths, hidden_in, w_value, w_key, w_query, eq, sel)

    mixed, quad, state_low, nquad, nlow = pl.pallas_call(
        functools.partial(finish, (nz, ny, nc, nx, prompts)),
        out_shape=(
            array(prompts, span, HL * HD, kind=BF16),
            array(1, prompts, HL * nx, own, HD),
            array(1, prompts, FD + 1, HL, HD),
            array(1, prompts, HL * nx, own),
            array(1, prompts, HL, FD + 1),
        ),
        in_specs=[scalars] + [whole] * 3 + [hbm] * 2,
        out_specs=(hbm,) * 5,
        scratch_shapes=[
            vmem(2 * own, part), vmem(own, ROWS), vmem(prompts + 1, HL * nx, own, HD, kind=F32), vmem(prompts, FD + 1, HL, HD, kind=F32),
            vmem(prompts, HL * nx, own, kind=F32), vmem(prompts, HL, FD + 1, kind=F32),
            dma((2,)), dma((5 * prompts,)),
        ],
        compiler_params=pltpu.CompilerParams(vmem_limit_bytes=LIMIT2),
        name="finish",
    )(owners, scaled, fx, low, spread, pick)
    return mixed, quad, jnp.transpose(state_low, (0, 1, 3, 2, 4)), nquad, nlow


def torus_of(mesh, shape=(8, 4, 2, 4)):
    return Mesh(mesh.devices.reshape(shape), ("z", "y", "c", "x"))


def run_on(torus):
    return jax.shard_map(
        body,
        mesh=torus,
        in_specs=(P(None, SEQ, None), P(), P(), P(None, "x"), P(), P()),
        out_specs=(
            P(None, SEQ, "x"),
            P(SEQ, None, None, "x", None),
            P(SEQ, None, "x", None, None),
            P(SEQ, None, None, "x"),
            P(SEQ, None, "x", None),
        ),
        check_vma=False,
    )


def solution(mesh):
    ny, nc = 4, 2
    feat = mesh.shape["feat"]
    return run_on(torus_of(mesh, (mesh.shape["seq"] // (ny * nc), ny, nc, feat)))
```
